32 devices in a mesh: row: 4 (over z), col: 4 (over y, x), layer: 2 (over core).
Axes of the slice: x: 2, y: 2, z: 4, core: 2. Of those that a mesh axis runs over, the one named last changes fastest.
Arguments:
- wavefunction: float32 [4096, 4096], P('row', 'col'), may hold values from -0.015625 to 1.515625
- start_block: float32 [4096, 2048], P(('col', 'layer'), 'row'), may hold values from -6 to 6
Outputs:
- basis: float32 [4096, 2048], P(('col', 'layer'), 'row')
The draws below stay inside these ranges and needn't reach their ends.
All inputs are finite; a program needn't handle non-finite values.
Results may differ from the reference program's by a relative error of at most 0.0003.
Values sent between devices are 32-bit elements; how exact they have to be, the bound alone decides.
No kernel may reach another device: no remote copies, remote signals or barrier semaphores. Data moves between devices by JAX's collectives and lax.ppermute only.
A program may use at most 128 MiB of HBM per device.

```python
import math
import jax
import jax.numpy as jnp
from jax import lax

M = 4096
K = 2048
ITERS = 1


def draw_wavefunction(key, part):
    first_key, second_key = jax.random.split(jax.random.fold_in(key, 17))
    scales = jnp.exp(jax.random.uniform(first_key, (M,), jnp.float32, 0.0, math.log(1.5)))
    noise = jnp.clip(jax.random.normal(second_key, (M, M), jnp.float32), -4.0, 4.0)
    return jnp.diag(scales) + 0.25 / math.sqrt(M) * noise


def shard_levels(stream_key, extent, shards, smallest, largest):
    gain, own = 1.0, jax.random.fold_in(stream_key, 6)
    for position, shards_of in shards:
        steps = jnp.exp(jax.random.uniform(jax.random.fold_in(own, position), (shards_of,), jnp.float32, smallest / len(shards), largest / len(shards)))
        gain = gain * jnp.repeat(steps, extent[position] // shards_of).reshape([-1 if axis == position else 1 for axis in range(len(extent))])
    return gain


def centred(stream_key, shape, deviation, most, shards=(), dtype=jnp.bfloat16):
    gain = shard_levels(stream_key, shape, shards, -0.22, 0.18) if shards else 1.0
    values = jax.random.normal(stream_key, shape, jnp.float32) * deviation * gain
    return jnp.minimum(jnp.maximum(values, -most), most).astype(dtype)


def setup_inputs(seed: int = 0) -> dict:
    arg_keys = jax.random.split(jax.random.key(seed), 3)
    return {
        "wavefunction": draw_wavefunction(jax.random.fold_in(arg_keys[2], 71), 0),
        "start_block": centred(arg_keys[1], (M, K), 1.0, 6.0, ((0, 8), (1, 4)), jnp.float32),
    }


def reference(wavefunction, start_block):
    density = jnp.dot(wavefunction.astype(jnp.float32), wavefunction.T.astype(jnp.float32), precision=lax.Precision.HIGHEST, preferred_element_type=jnp.float32)
    current = start_block
    for iteration in range(ITERS):
        image_block = jnp.dot(density.astype(jnp.float32), current.astype(jnp.float32), precision=lax.Precision.HIGHEST, preferred_element_type=jnp.float32)
        gram_matrix = jnp.dot(image_block.T.astype(jnp.float32), image_block.astype(jnp.float32), precision=lax.Precision.HIGHEST, preferred_element_type=jnp.float32)
        factor = jnp.linalg.cholesky(gram_matrix)
        current = jax.scipy.linalg.solve_triangular(factor, image_block.T, lower=True).T
    return current * math.sqrt(M)
```

```python
import functools, math
import jax, jax.numpy as jnp
from jax import lax
from jax.experimental import pallas as pl
from jax.experimental.pallas import tpu as pltpu
from jax.sharding import PartitionSpec as P
F32, BF16 = jnp.float32, jnp.bfloat16
NN = (((1,), (0,)), ((), ()))
NT = (((1,), (1,)), ((), ()))
TN = (((0,), (0,)), ((), ()))
STEPS = 5


def mm(a, b, dims):
    return lax.dot_general(a, b, dims, preferred_element_type=F32)


def split(x):
    high = x.astype(BF16)
    return high, (x - high.astype(F32)).astype(BF16)


def mm3(a, b, dims):
    return mm(a[0], b[0], dims) + (mm(a[0], b[1], dims) + mm(a[1], b[0], dims))


def iotas(n):
    return lax.broadcasted_iota(jnp.int32, (n, n), 0), lax.broadcasted_iota(jnp.int32, (n, n), 1)


def lower_half(x, rows, cols):
    return jnp.where(rows > cols, x, jnp.where(rows == cols, 0.5 * x, 0.0))


def inverse_factor(block, out_ref, work_ref):
    n = block.shape[0]
    rows, cols = iotas(n)
    eye = (rows == cols).astype(F32)
    on_diag = block * eye
    scale_row = lax.rsqrt(jnp.sum(on_diag, axis=0, keepdims=True))
    scale_col = lax.rsqrt(jnp.sum(on_diag, axis=1, keepdims=True))
    scaled = block * scale_row * scale_col
    w = scaled
    half = lower_half(w - eye, rows, cols)
    x = eye - half
    hb = half.astype(BF16)
    w = w - mm(hb, w.astype(BF16), NN)
    w = w - mm(w.astype(BF16), hb, NT)
    for _ in range(STEPS - 1):
        hb = lower_half(w - eye, rows, cols).astype(BF16)
        x = x - mm(hb, x.astype(BF16), NN)
        w = w - mm(hb, w.astype(BF16), NN)
        w = w - mm(w.astype(BF16), hb, NT)
    xs = split(x)
    error = mm3(split(mm3(xs, split(scaled), NN)), xs, NT) - eye
    x = x - mm3(split(lower_half(error, rows, cols)), xs, NN)
    out_ref[...] = x * scale_row
    size = jnp.sum(error * error)

    @pl.when(jnp.logical_not(size < 1e-3))
    def _():
        work_ref[...] = block
        out_ref[...] = eye

        @pl.loop(0, n)
        def _(j):
            state = work_ref[...]
            factors = out_ref[...]
            column = jnp.sum(jnp.where(cols == j, state, 0.0), axis=1, keepdims=True)
            below = lax.broadcasted_iota(jnp.int32, (n, 1), 0)
            pivot = jnp.sum(jnp.where(below == j, column, 0.0), axis=0, keepdims=True)
            multiplier = jnp.where(below > j, column / pivot, 0.0)
            work_ref[...] = state - multiplier * work_ref[pl.ds(j, 1), :]
            out_ref[...] = factors - multiplier * out_ref[pl.ds(j, 1), :]

        pivots = jnp.sum(work_ref[...] * eye, axis=1, keepdims=True)
        out_ref[...] = out_ref[...] * lax.rsqrt(pivots)


def packed(i, j, blocks):
    return j * blocks - (j * (j - 1)) // 2 + (i - j)


def factor_kernel(blocks, size, pieces, panels, scale, me_ref, order_ref, *refs):
    g_pieces = refs[:pieces]
    b_pieces = refs[pieces:pieces + panels]
    out_ref, g, b, ph, plo, x_ref, work_ref, sem = refs[pieces + panels:]
    me = me_ref[0]
    per = blocks // panels
    piece_rows = g_pieces[0].shape[0]
    copies = []
    for s in range(pieces):
        start = pl.multiple_of(order_ref[s] * piece_rows, 8)
        copies.append(pltpu.make_async_copy(g_pieces[s], g.at[pl.ds(start, piece_rows), :], sem.at[s]))
    for s in range(panels):
        panel = lax.rem(me - s + panels, panels)
        for h in range(per):
            copies.append(pltpu.make_async_copy(
                b_pieces[s].at[:, pl.ds(h * size, size)], b.at[panel * per + h], sem.at[pieces + s * per + h]))
    for c in copies:
        c.start()
    for c in copies:
        c.wait()
    count = (me + 1) * per

    def block_at(i, j):
        return pl.ds(pl.multiple_of(packed(i, j, blocks) * size, size), size)

    @pl.loop(0, count)
    def _(k):
        inverse_factor(g[block_at(k, k), :], x_ref, work_ref)
        xs = split(x_ref[...])
        done = mm3(split(b[k]), xs, NT)
        ys = split(done)

        @pl.when(k >= me * per)
        def _():
            out_ref[k - me * per] = done * scale

        @pl.loop(k + 1, count)
        def _(i):
            hi, lo = split(mm3(split(g[block_at(i, k), :]), xs, NT))
            ph[i] = hi
            plo[i] = lo

        @pl.loop(k + 1, count)
        def _(j):
            right = (ph[j], plo[j])
            b[j] = b[j] - mm3(ys, right, NT)

            @pl.loop(j, count)
            def _(i):
                where = block_at(i, j)
                g[where, :] = g[where, :] - mm3((ph[i], plo[i]), right, NT)


def factor_apply(me, order, g_pieces, b_pieces, size, scale):
    rows, width = b_pieces[0].shape
    panels = len(b_pieces)
    per = width // size
    blocks = panels * per
    n_sem = len(g_pieces) + panels * per
    any_spec = pl.BlockSpec(memory_space=pl.ANY)
    smem = pl.BlockSpec(memory_space=pltpu.SMEM)
    total = blocks * (blocks + 1) // 2
    out = pl.pallas_call(
        functools.partial(factor_kernel, blocks, size, len(g_pieces), panels, scale),
        out_shape=jax.ShapeDtypeStruct((per, rows, size), F32),
        in_specs=[smem, smem] + [any_spec] * (len(g_pieces) + panels),
        out_specs=pl.BlockSpec(memory_space=pltpu.VMEM),
        scratch_shapes=[
            pltpu.VMEM((total * size, size), F32),
            pltpu.VMEM((blocks, rows, size), F32),
            pltpu.VMEM((blocks, size, size), BF16),
            pltpu.VMEM((blocks, size, size), BF16),
            pltpu.VMEM((size, size), F32),
            pltpu.VMEM((size, size), F32),
            pltpu.SemaphoreType.DMA((n_sem,)),
        ],
        compiler_params=pltpu.CompilerParams(vmem_limit_bytes=56 * 1024 * 1024),
        cost_estimate=pl.CostEstimate(flops=6 * 10**10, bytes_accessed=2 * 10**7, transcendentals=0),
        name="factor",
    )(me, order, *g_pieces, *b_pieces)
    return out.transpose(1, 0, 2).reshape(rows, width)


def gram_kernel(panels, per, size, me_ref, row_ref, col_ref, *refs):
    pieces = refs[:panels]
    out_ref, hi, lo = refs[panels:]
    t = pl.program_id(0)

    @pl.when(t == 0)
    def _():
        for s in range(panels):
            panel = lax.rem(me_ref[0] - s + panels, panels)
            for h in range(per):
                high, low = split(pieces[s][:, h * size:(h + 1) * size])
                hi[panel * per + h] = high
                lo[panel * per + h] = low

    i, j = row_ref[t], col_ref[t]
    out_ref[...] = mm3((hi[i], lo[i]), (hi[j], lo[j]), TN)


def packed_gram(me, pieces, size):
    rows, width = pieces[0].shape
    panels = len(pieces)
    per = width // size
    blocks = panels * per
    pairs = [(i, j) for j in range(blocks) for i in range(j, blocks)]
    row_of = jnp.array([p[0] for p in pairs], jnp.int32)
    col_of = jnp.array([p[1] for p in pairs], jnp.int32)
    whole = pl.BlockSpec((rows, width), lambda t, *_: (0, 0))
    return pl.pallas_call(
        functools.partial(gram_kernel, panels, per, size),
        out_shape=jax.ShapeDtypeStruct((len(pairs) * size, size), F32),
        grid_spec=pltpu.PrefetchScalarGridSpec(
            num_scalar_prefetch=3,
            grid=(len(pairs),),
            in_specs=[whole] * panels,
            out_specs=pl.BlockSpec((size, size), lambda t, *_: (t, 0)),
            scratch_shapes=[pltpu.VMEM((blocks, rows, size), BF16)] * 2,
        ),
        cost_estimate=pl.CostEstimate(flops=6 * len(pairs) * rows * size * size, bytes_accessed=len(pairs) * size * size * 4, transcendentals=0),
        name="gram",
    )(me, row_of, col_of, *pieces)


def dot3(left, right, dims):
    return lax.dot_general(left, right, dims, precision=lax.Precision.HIGH, preferred_element_type=F32)


def take(x, index, axis=0):
    return lax.dynamic_index_in_dim(x, index, axis, keepdims=False)


def shift_by_xor(x, axis, step):
    n = lax.axis_size(axis)
    return lax.ppermute(x, axis, [(a, a ^ step) for a in range(n)])


def scatter_sum(x, axis):
    me, n = lax.axis_index(axis), lax.axis_size(axis)
    received = [shift_by_xor(take(x, me ^ s), axis, s) for s in range(1, n)]
    return sum(received, take(x, me))


def own_and_others(x, axis):
    return [x] + [shift_by_xor(x, axis, s) for s in range(1, lax.axis_size(axis))]


def ordered(parts, axis):
    me = lax.axis_index(axis)
    out = jnp.zeros((len(parts),) + parts[0].shape, parts[0].dtype)
    for s, part in enumerate(parts):
        out = lax.dynamic_update_index_in_dim(out, part, me ^ s, 0)
    return out


def chain(x, axis, direction):
    n = lax.axis_size(axis)
    pairs = [(a, a + direction) for a in range(n) if 0 <= a + direction < n]
    got = [x]
    for _ in range(n - 1):
        got.append(lax.ppermute(got[-1], axis, pairs))
    return got


def shards(wavefunction, start_block):
    rows_n, cols_n, layers = (lax.axis_size(a) for a in ("row", "col", "layer"))
    row, col, layer = (lax.axis_index(a) for a in ("row", "col", "layer"))
    order_m = wavefunction.shape[0] * rows_n
    per_row, panel = start_block.shape
    size = min(256, panel)

    width = wavefunction.shape[1] // layers
    own = lax.dynamic_slice_in_dim(wavefunction, layer * width, width, 1)
    up, down = chain(own, "row", 1), chain(own, "row", -1)
    start = ordered(own_and_others(ordered(own_and_others(start_block, "col"), "col"), "layer"), "layer")
    start = start.transpose(1, 0, 2, 3).reshape(rows_n, -1, panel)

    psi = jnp.zeros((rows_n,) + own.shape, F32)
    psi = lax.dynamic_update_index_in_dim(psi, own, row, 0)
    for s in range(1, rows_n):
        block = jnp.where(row >= s, up[s], down[rows_n - s])
        psi = lax.dynamic_update_index_in_dim(psi, block, (row - s) % rows_n, 0)
    psi = psi.reshape(order_m, width)
    inner = dot3(psi, start.reshape(order_m, panel), TN)
    image = dot3(psi, inner, NN).reshape(cols_n, layers, per_row, panel)
    image = scatter_sum(scatter_sum(image.transpose(1, 0, 2, 3), "layer"), "col")

    panels = chain(image, "row", 1)
    me = row.reshape(1).astype(jnp.int32)
    gram = packed_gram(me, panels, size)
    gram = gram.reshape(layers, cols_n, -1, size)
    gram = scatter_sum(scatter_sum(gram, "layer"), "col")
    pieces, places = [], []
    for s, part in enumerate(own_and_others(gram, "col")):
        for t, piece in enumerate(own_and_others(part, "layer")):
            pieces.append(piece)
            places.append((layer ^ t) * cols_n + (col ^ s))
    return factor_apply(me, jnp.stack(places).astype(jnp.int32), pieces, panels, size, math.sqrt(order_m))


def solution(mesh):
    placed = (P("row", "col"), P(("col", "layer"), "row"))
    return jax.shard_map(
        shards, mesh=mesh, in_specs=placed, out_specs=P(("col", "layer"), "row"), check_vma=False
    )
```

```python
import functools, math
import jax, jax.numpy as jnp
from jax import lax
from jax.experimental import pallas as pl
from jax.experimental.pallas import tpu as pltpu
from jax.sharding import PartitionSpec as P

F32, BF16 = jnp.float32, jnp.bfloat16
NN = (((1,), (0,)), ((), ()))
NT = (((1,), (1,)), ((), ()))
TN = (((0,), (0,)), ((), ()))
STEPS = 5


def mm(a, b, dims):
    return lax.dot_general(a, b, dims, preferred_element_type=F32)


def split(x):
    high = x.astype(BF16)
    return high, (x - high.astype(F32)).astype(BF16)


def mm3(a, b, dims):
    return mm(a[0], b[0], dims) + (mm(a[0], b[1], dims) + mm(a[1], b[0], dims))


def iotas(n):
    return lax.broadcasted_iota(jnp.int32, (n, n), 0), lax.broadcasted_iota(jnp.int32, (n, n), 1)


def lower_half(x, rows, cols):
    return jnp.where(rows > cols, x, jnp.where(rows == cols, 0.5 * x, 0.0))


def inverse_factor(block, out_ref, work_ref):
    n = block.shape[0]
    rows, cols = iotas(n)
    eye = (rows == cols).astype(F32)
    on_diag = block * eye
    scale_row = lax.rsqrt(jnp.sum(on_diag, axis=0, keepdims=True))
    scale_col = lax.rsqrt(jnp.sum(on_diag, axis=1, keepdims=True))
    scaled = block * scale_row * scale_col
    w = scaled
    half = lower_half(w - eye, rows, cols)
    x = eye - half
    hb = half.astype(BF16)
    w = w - mm(hb, w.astype(BF16), NN)
    w = w - mm(w.astype(BF16), hb, NT)
    for _ in range(STEPS - 1):
        hb = lower_half(w - eye, rows, cols).astype(BF16)
        x = x - mm(hb, x.astype(BF16), NN)
        w = w - mm(hb, w.astype(BF16), NN)
        w = w - mm(w.astype(BF16), hb, NT)
    xs = split(x)
    error = mm3(split(mm3(xs, split(scaled), NN)), xs, NT) - eye
    x = x - mm3(split(lower_half(error, rows, cols)), xs, NN)
    out_ref[...] = x * scale_row
    size = jnp.sum(error * error)

    @pl.when(jnp.logical_not(size < 1e-3))
    def _():
        work_ref[...] = block
        out_ref[...] = eye

        @pl.loop(0, n)
        def _(j):
            state = work_ref[...]
            factors = out_ref[...]
            column = jnp.sum(jnp.where(cols == j, state, 0.0), axis=1, keepdims=True)
            below = lax.broadcasted_iota(jnp.int32, (n, 1), 0)
            pivot = jnp.sum(jnp.where(below == j, column, 0.0), axis=0, keepdims=True)
            multiplier = jnp.where(below > j, column / pivot, 0.0)
            work_ref[...] = state - multiplier * work_ref[pl.ds(j, 1), :]
            out_ref[...] = factors - multiplier * out_ref[pl.ds(j, 1), :]

        pivots = jnp.sum(work_ref[...] * eye, axis=1, keepdims=True)
        out_ref[...] = out_ref[...] * lax.rsqrt(pivots)


def factor_kernel(blocks, size, groups, bundles, shares, swaps, scale, me_ref, order_ref, *refs):
    per = blocks // groups
    width = per * size
    arrays = shares + swaps
    g_refs = [refs[n * arrays:(n + 1) * arrays] for n in range(len(bundles))]
    refs = refs[len(bundles) * arrays:]
    b_refs = [refs[s * per:(s + 1) * per] for s in range(groups)]
    out_ref, g, b, left3, right3, x_ref, work_ref, sem = refs[groups * per:]
    me = me_ref[0]
    pieces = shares * (1 + swaps)
    copies = [[] for _ in range(groups)]
    n_sem = 0
    for bundle, arrays_in in zip(bundles, g_refs):
        for t in range(pieces):
            piece = arrays_in[t] if t < shares else arrays_in[shares + t // shares - 1].at[t % shares]
            first = 0
            for s in bundle:
                rows = (s + 1) * width // pieces
                start = pl.multiple_of((me - s) * width + order_ref[t] * rows, 8)
                for h in range(per):
                    copies[s].append(pltpu.make_async_copy(
                        piece.at[pl.ds(first, rows), pl.ds(h * size, size)],
                        g.at[(me - s) * per + h, pl.ds(start, rows), :], sem.at[n_sem]))
                    n_sem += 1
                first += rows
    for s in range(groups):
        for h in range(per):
            copies[s].append(pltpu.make_async_copy(b_refs[s][h], b.at[(me - s) * per + h], sem.at[n_sem]))
            n_sem += 1

    def each_group(wanted, act):
        for s in range(groups):
            @pl.when(wanted(s))
            def _():
                for c in copies[s]:
                    act(c)

    each_group(lambda s: s == me, lambda c: c.start())
    each_group(lambda s: s < me, lambda c: c.start())
    each_group(lambda s: s == me, lambda c: c.wait())
    count = (me + 1) * per

    def rows_of(i):
        return pl.ds(pl.multiple_of(i * size, size), size)

    @pl.loop(0, count)
    def _(k):
        inverse_factor(g[k, rows_of(k), :], x_ref, work_ref)
        xs = split(x_ref[...])

        @pl.when(k == 0)
        def _():
            each_group(lambda s: s < me, lambda c: c.wait())

        done = mm3(split(b[k]), xs, NT)
        high, low = split(done)
        done3 = jnp.concatenate([high, high, low], axis=1)

        @pl.when(k >= me * per)
        def _():
            out_ref[:, pl.ds(pl.multiple_of((k - me * per) * size, size), size)] = done * scale

        @pl.loop(k + 1, count)
        def _(i):
            hi, lo = split(mm3(split(g[k, rows_of(i), :]), xs, NT))
            left3[i] = jnp.concatenate([hi, hi, lo], axis=1)
            right3[i] = jnp.concatenate([hi, lo, hi], axis=1)

        @pl.loop(k + 1, count)
        def _(j):
            right = right3[j]
            b[j] = b[j] - mm(done3, right, NT)

            @pl.loop(j, count)
            def _(i):
                g[j, rows_of(i), :] = g[j, rows_of(i), :] - mm(left3[i], right, NT)


def factor_apply(me, order, bundles, g_arrays, shares, b_groups, size, scale):
    groups, per = len(b_groups), len(b_groups[0])
    swaps = len(g_arrays[0]) - shares
    rows = b_groups[0][0].shape[0]
    blocks = groups * per
    any_spec = pl.BlockSpec(memory_space=pl.ANY)
    smem = pl.BlockSpec(memory_space=pltpu.SMEM)
    arrays = sum(g_arrays, []) + sum(b_groups, [])
    return pl.pallas_call(
        functools.partial(factor_kernel, blocks, size, groups, bundles, shares, swaps, scale),
        out_shape=jax.ShapeDtypeStruct((rows, per * size), F32),
        in_specs=[smem, smem] + [any_spec] * len(arrays),
        out_specs=pl.BlockSpec(memory_space=pltpu.VMEM),
        scratch_shapes=[
            pltpu.VMEM((blocks, blocks * size, size), F32),
            pltpu.VMEM((blocks, rows, size), F32),
            pltpu.VMEM((blocks, size, 3 * size), BF16),
            pltpu.VMEM((blocks, size, 3 * size), BF16),
            pltpu.VMEM((size, size), F32),
            pltpu.VMEM((size, size), F32),
            pltpu.SemaphoreType.DMA((groups * per * (shares * (1 + swaps) + 1),)),
        ],
        compiler_params=pltpu.CompilerParams(vmem_limit_bytes=56 * 1024 * 1024),
        cost_estimate=pl.CostEstimate(flops=6 * 10**10, bytes_accessed=2 * 10**7, transcendentals=0),
        name="factor",
    )(me, order, *arrays)


def image_call(places, s_places, blocks, starts, sizes, per, inner=None):
    last = inner is not None
    rows_n, cols_n, layers = sizes
    cut, wide = blocks[0][0].shape
    cuts = len(blocks[0])
    rows_s, panel = starts[0].shape
    any_spec = pl.BlockSpec(memory_space=pl.ANY)
    smem = pl.BlockSpec(memory_space=pltpu.SMEM)
    vmem = pl.BlockSpec(memory_space=pltpu.VMEM)
    scratch = [
        pltpu.VMEM((rows_n, cuts * cut, wide), F32),
        pltpu.VMEM((rows_n * layers, rows_s, panel), F32),
        pltpu.SemaphoreType.DMA((len(blocks) * cuts + len(starts),)),
    ]
    flat = sum(blocks, [])
    if last:
        shape = [jax.ShapeDtypeStruct((cols_n, rows_s, panel // per), F32)] * (per * layers)
        spec = [any_spec] * (per * layers)
        scratch += [
            pltpu.VMEM((wide, panel), F32),
            pltpu.VMEM((rows_n, layers, rows_s, panel), F32),
            pltpu.SemaphoreType.DMA((rows_n, layers, per)),
        ]
        flops = 6 * wide * panel * cuts * cut * (rows_n + 1)
    else:
        shape, spec = jax.ShapeDtypeStruct((wide, panel), F32), vmem
        flops = 6 * wide * panel * cuts * cut * (rows_n - 1)
    return pl.pallas_call(
        functools.partial(image_kernel, sizes, cuts, per, last),
        out_shape=shape,
        in_specs=[smem, smem] + [any_spec] * (len(flat) + len(starts)) + [vmem] * last,
        out_specs=spec,
        scratch_shapes=scratch,
        compiler_params=pltpu.CompilerParams(vmem_limit_bytes=56 * 1024 * 1024),
        cost_estimate=pl.CostEstimate(flops=flops, bytes_accessed=4 * cuts * cut * wide * rows_n, transcendentals=0),
        name="image" if last else "inner",
    )(places, s_places, *flat, *starts, *([inner] if last else []))


def image_kernel(sizes, cuts, per, last, place_ref, s_place_ref, *refs):
    rows_n, cols_n, layers = sizes
    far = rows_n - 1
    hops = [0]
    for step in range(1, rows_n if last else far):
        hops += [-step, step]
    n_a, shares = len(hops) * cuts, cols_n * layers
    a_refs, s_refs, refs = refs[:n_a], refs[n_a:n_a + shares], refs[n_a + shares:]
    if last:
        outs = refs[1:1 + per * layers]
        a, s, sem, acc, o, out_sem = refs[1 + per * layers:]
    else:
        acc, a, s, sem = refs
    me, col, layer = place_ref[0], place_ref[1], place_ref[2]
    cut = a_refs[0].shape[0]
    rows_s, panel = s_refs[0].shape
    size = panel // per

    def each_block(z, act):
        for n in range(n_a):
            @pl.when(me + hops[n // cuts] == z)
            def _():
                act(pltpu.make_async_copy(
                    a_refs[n], a.at[z, pl.ds(n % cuts * cut, cut), :], sem.at[n]))

    def each_share(z, act):
        for n in range(shares):
            @pl.when(s_place_ref[n] // layers == z)
            def _():
                act(pltpu.make_async_copy(s_refs[n], s.at[s_place_ref[n]], sem.at[n_a + n]))

    def rows_of(m):
        return pl.ds(pl.multiple_of(m * rows_s, rows_s), rows_s)

    def add_product(z):
        each_block(z, lambda c: c.wait())
        each_share(z, lambda c: c.wait())

        @pl.loop(0, layers)
        def _(m):
            acc[...] += mm3(split(a[z, rows_of(m), :]), split(s[z * layers + m]), TN)

    if not last:
        acc[...] = jnp.zeros_like(acc)

        @pl.loop(0, rows_n)
        def _(step):
            z = lax.rem(me + step, rows_n)
            each_block(z, lambda c: c.start())

            @pl.when(jnp.abs(z - me) < far)
            def _():
                each_share(z, lambda c: c.start())

        @pl.loop(0, rows_n)
        def _(step):
            z = lax.rem(me + step, rows_n)

            @pl.when(jnp.abs(z - me) < far)
            def _():
                add_product(z)

        return

    def each_out(z, m, act):
        for x in range(layers):
            @pl.when(jnp.bitwise_xor(m, layer) == x)
            def _():
                for h in range(per):
                    act(pltpu.make_async_copy(
                        o.at[z, m, :, pl.ds(h * size, size)],
                        outs[x * per + h].at[jnp.bitwise_xor(z, col)], out_sem.at[z, m, h]))

    far_z = far - me
    ends = jnp.abs(far_z - me) == far

    @pl.when(ends)
    def _():
        each_block(far_z, lambda c: c.start())
        each_share(far_z, lambda c: c.start())

    @pl.loop(0, rows_n)
    def _(z):
        @pl.when(jnp.abs(z - me) < far)
        def _():
            each_block(z, lambda c: c.start())

    acc[...] = refs[0][...]

    @pl.when(ends)
    def _():
        add_product(far_z)

    inner = split(acc[...])

    @pl.loop(0, rows_n)
    def _(z):
        @pl.when(jnp.abs(z - me) < far)
        def _():
            each_block(z, lambda c: c.wait())

        @pl.loop(0, layers)
        def _(m):
            o[z, m] = mm3(split(a[z, rows_of(m), :]), inner, NN)
            each_out(z, m, lambda c: c.start())

    @pl.loop(0, rows_n)
    def _(z):
        @pl.loop(0, layers)
        def _(m):
            each_out(z, m, lambda c: c.wait())


def gram_kernel(bundle, sizes, per, place_ref, *refs):
    cols_n, layers = sizes
    shares = cols_n * layers
    n_p = (bundle[-1] + 1) * per
    p_refs, outs, (left3, right3, g, sem) = refs[:n_p], refs[n_p:n_p + layers], refs[n_p + layers:]
    rows, size = p_refs[0].shape
    width = size * per
    col, layer = place_ref[1], place_ref[2]
    for t in range(bundle[-1] + 1):
        for h in range(per):
            hi, lo = split(p_refs[t * per + h][...])
            here = pl.ds(h * size, size)
            for n, part in enumerate((hi, hi, lo)):
                left3[t, n * rows:(n + 1) * rows, here] = part
            if t in bundle:
                for n, part in enumerate((hi, lo, hi)):
                    right3[bundle.index(t), n * rows:(n + 1) * rows, here] = part
    base, first = 0, 0
    copies = []
    for i, s in enumerate(bundle):
        for t in range(s, -1, -1):
            at = base + (s - t) * width
            g[at:at + width, :] = mm(left3[t], right3[i], TN)
        n = (s + 1) * width // shares
        for x in range(layers):
            for y in range(cols_n):
                share = jnp.bitwise_xor(layer, x) * cols_n + jnp.bitwise_xor(col, y)
                start = pl.multiple_of(base + share * n, 8)
                copies.append(pltpu.make_async_copy(
                    g.at[pl.ds(start, n), :], outs[x].at[y, pl.ds(first, n), :], sem.at[len(copies)]))
                copies[-1].start()
        base += (s + 1) * width
        first += n
    for c in copies:
        c.wait()


def gram_call(place, bundle, panels, sizes):
    cols_n, layers = sizes
    per = len(panels[0])
    rows, size = panels[0][0].shape
    width = size * per
    total = sum(s + 1 for s in bundle) * width
    flat = sum(panels[:bundle[-1] + 1], [])
    vmem = pl.BlockSpec(memory_space=pltpu.VMEM)
    return pl.pallas_call(
        functools.partial(gram_kernel, bundle, sizes, per),
        out_shape=[jax.ShapeDtypeStruct((cols_n, total // (cols_n * layers), width), F32)] * layers,
        in_specs=[pl.BlockSpec(memory_space=pltpu.SMEM)] + [vmem] * len(flat),
        out_specs=[pl.BlockSpec(memory_space=pl.ANY)] * layers,
        scratch_shapes=[
            pltpu.VMEM((bundle[-1] + 1, 3 * rows, width), BF16),
            pltpu.VMEM((len(bundle), 3 * rows, width), BF16),
            pltpu.VMEM((total, width), F32),
            pltpu.SemaphoreType.DMA((len(bundle) * cols_n * layers,)),
        ],
        compiler_params=pltpu.CompilerParams(vmem_limit_bytes=48 * 1024 * 1024),
        cost_estimate=pl.CostEstimate(flops=6 * total * width * rows, bytes_accessed=4 * total * width, transcendentals=0),
        name="gram",
    )(place, *flat)


def shift_by_xor(x, axis, step):
    n = lax.axis_size(axis)
    return lax.ppermute(x, axis, [(a, a ^ step) for a in range(n)])


def own_and_others(x, axis):
    return [x] + [shift_by_xor(x, axis, s) for s in range(1, lax.axis_size(axis))]


def chain(x, axis, direction):
    n = lax.axis_size(axis)
    pairs = [(a, a + direction) for a in range(n) if 0 <= a + direction < n]
    got = [x]
    for _ in range(n - 1):
        got.append(lax.ppermute(got[-1], axis, pairs))
    return got


def exchange_sum(parts, axis):
    came = [shift_by_xor(parts[s], axis, s) for s in range(1, len(parts))]
    return sum(came, parts[0])


def shards(wavefunction, start_block):
    sizes = rows_n, cols_n, layers = tuple(lax.axis_size(a) for a in ("row", "col", "layer"))
    row, col, layer = (lax.axis_index(a).astype(jnp.int32) for a in ("row", "col", "layer"))
    order_m = wavefunction.shape[0] * rows_n
    panel = start_block.shape[1]
    size = min(256, panel)
    per = panel // size
    place = jnp.stack([row, col, layer])

    width = wavefunction.shape[1] // layers
    own = lax.dynamic_slice_in_dim(wavefunction, layer * width, width, 1)
    chains = [(chain(cut, "row", 1), chain(cut, "row", -1)) for cut in jnp.split(own, 2)]
    blocks = [[c[0][0] for c in chains]]
    for s in range(1, rows_n):
        blocks += [[c[0][s] for c in chains], [c[1][s] for c in chains]]
    starts, s_places = [], []
    for s, part in enumerate(own_and_others(start_block, "col")):
        for t, piece in enumerate(own_and_others(part, "layer")):
            starts.append(piece)
            s_places.append((col ^ s) * layers + (layer ^ t))
    s_places = jnp.stack(s_places)
    inner = image_call(place, s_places, blocks[:-2], starts, sizes, per)
    images = image_call(place, s_places, blocks, starts, sizes, per, inner)
    panels = [[]]
    for h in range(per):
        image = exchange_sum([images[x * per + h] for x in range(layers)], "layer")
        panels[0].append(exchange_sum([image[s] for s in range(cols_n)], "col"))

    bundles = [[0, 1]] + [[s] for s in range(2, rows_n)]
    up = [(a, a + 1) for a in range(rows_n - 1)]
    g_arrays = []
    for s in range(rows_n):
        if s:
            panels.append([lax.ppermute(part, "row", up) for part in panels[-1]])
        for bundle in bundles:
            if bundle[-1] == s:
                gram = gram_call(place, bundle, panels, (cols_n, layers))
                gram = exchange_sum(gram, "layer")
                gram = [gram[y] for y in range(cols_n)]
                gram = exchange_sum(gram, "col")
                pieces = own_and_others(gram, "col")
                stack = jnp.stack(pieces)
                g_arrays.append(pieces + own_and_others(stack, "layer")[1:])
    places = jnp.stack([(layer ^ x) * cols_n + (col ^ s) for x in range(layers) for s in range(cols_n)])
    return factor_apply(place, places, bundles, g_arrays, cols_n, panels, size, math.sqrt(order_m))


def solution(mesh):
    placed = (P("row", "col"), P(("col", "layer"), "row"))

    return jax.shard_map(
        shards, mesh=mesh, in_specs=placed, out_specs=P(("col", "layer"), "row"), check_vma=False
    )
```

```python
import functools, math
import jax, jax.numpy as jnp
from jax import lax
from jax.experimental import pallas as pl
from jax.experimental.pallas import tpu as pltpu
from jax.sharding import PartitionSpec as P

F32, BF16 = jnp.float32, jnp.bfloat16
NN = (((1,), (0,)), ((), ()))
NT = (((1,), (1,)), ((), ()))
TN = (((0,), (0,)), ((), ()))
STEPS = 5
BESIDE = 2


def mm(a, b, dims):
    return lax.dot_general(a, b, dims, preferred_element_type=F32)


def split(x):
    high = x.astype(BF16)
    return high, (x - high.astype(F32)).astype(BF16)


def mm3(a, b, dims):
    return mm(a[0], b[0], dims) + (mm(a[0], b[1], dims) + mm(a[1], b[0], dims))


def iotas(n):
    return lax.broadcasted_iota(jnp.int32, (n, n), 0), lax.broadcasted_iota(jnp.int32, (n, n), 1)


def lower_half(x, rows, cols):
    return jnp.where(rows > cols, x, jnp.where(rows == cols, 0.5 * x, 0.0))


def inverse_factor(block, out_ref, work_ref, beside):
    n = block.shape[0]
    rows, cols = iotas(n)
    eye = (rows == cols).astype(F32)
    on_diag = block * eye
    scale_row = lax.rsqrt(jnp.sum(on_diag, axis=0, keepdims=True))
    scale_col = lax.rsqrt(jnp.sum(on_diag, axis=1, keepdims=True))
    scaled = block * scale_row * scale_col
    w = scaled
    x = eye
    for step in range(STEPS):
        half = lower_half(w - eye, rows, cols)
        hb = half.astype(BF16)
        moved = mm(hb, w.astype(BF16), NN)
        x = x - (mm(hb, x.astype(BF16), NN) if step else half)
        beside()
        w = w - moved
        w = w - mm(w.astype(BF16), hb, NT)
        beside()
    xs = split(x)
    product = mm3(xs, split(scaled), NN)
    beside()
    error = mm3(split(product), xs, NT) - eye
    beside()
    x = x - mm3(split(lower_half(error, rows, cols)), xs, NN)
    beside()
    out_ref[...] = x * scale_row
    size = jnp.sum(error * error)

    @pl.when(jnp.logical_not(size < 1e-3))
    def _():
        work_ref[...] = block
        out_ref[...] = eye

        @pl.loop(0, n)
        def _(j):
            state = work_ref[...]
            factors = out_ref[...]
            column = jnp.sum(jnp.where(cols == j, state, 0.0), axis=1, keepdims=True)
            below = lax.broadcasted_iota(jnp.int32, (n, 1), 0)
            pivot = jnp.sum(jnp.where(below == j, column, 0.0), axis=0, keepdims=True)
            multiplier = jnp.where(below > j, column / pivot, 0.0)
            work_ref[...] = state - multiplier * work_ref[pl.ds(j, 1), :]
            out_ref[...] = factors - multiplier * out_ref[pl.ds(j, 1), :]

        pivots = jnp.sum(work_ref[...] * eye, axis=1, keepdims=True)
        out_ref[...] = out_ref[...] * lax.rsqrt(pivots)


def task_table(blocks, per, extra):
    lists = []
    for count in range(per, blocks + 1, per):
        mine = []
        for j in range(count - 1, 0, -1):
            mine += [(i, j) for i in list(range(j + 1, count)) + list(range(blocks, blocks + extra))] + [(j, j)]
        lists.append(mine)
    most = max(len(mine) for mine in lists) + 1
    idle = (blocks + extra, blocks - 1)
    return most, jnp.array([mine + [idle] * (most - len(mine)) for mine in lists], jnp.int32).reshape(-1)


def factor_kernel(blocks, size, groups, bundles, shares, swaps, scale, extra, most, me_ref, order_ref, table_ref, *refs):
    per = blocks // groups
    width = per * size
    arrays = shares + swaps
    g_refs = [refs[n * arrays:(n + 1) * arrays] for n in range(len(bundles))]
    refs = refs[len(bundles) * arrays:]
    b_refs = [refs[s * per:(s + 1) * per] for s in range(groups)]
    out_ref, g, left3, right3, x_ref, work_ref, sem = refs[groups * per:]
    tall = b_refs[0][0].shape[0]
    me = me_ref[0]
    pieces = shares * (1 + swaps)
    copies = [[] for _ in range(groups)]
    n_sem = 0
    for bundle, arrays_in in zip(bundles, g_refs):
        for t in range(pieces):
            piece = arrays_in[t] if t < shares else arrays_in[shares + t // shares - 1].at[t % shares]
            first = 0
            for s in bundle:
                rows = (s + 1) * width // pieces
                start = pl.multiple_of((me - s) * width + order_ref[t] * rows, 8)
                for h in range(per):
                    copies[s].append(pltpu.make_async_copy(
                        piece.at[pl.ds(first, rows), pl.ds(h * size, size)],
                        g.at[(me - s) * per + h, pl.ds(start, rows), :], sem.at[n_sem]))
                    n_sem += 1
                first += rows
    for s in range(groups):
        for h in range(per):
            copies[s].append(pltpu.make_async_copy(
                b_refs[s][h], g.at[(me - s) * per + h, pl.ds(blocks * size, tall), :], sem.at[n_sem]))
            n_sem += 1

    def each_group(wanted, act):
        for s in range(groups):
            @pl.when(wanted(s))
            def _():
                for c in copies[s]:
                    act(c)

    each_group(lambda s: s == me, lambda c: c.start())
    each_group(lambda s: s < me, lambda c: c.start())
    each_group(lambda s: s == me, lambda c: c.wait())
    count = (me + 1) * per

    def rows_of(i, n=1):
        return pl.ds(pl.multiple_of(i * size, size), n * size)

    def update(t, limit):
        at = 2 * (me * most + jnp.where(t < limit, t, most - 1))
        i, j = table_ref[at], table_ref[at + 1]
        g[j, rows_of(i), :] = g[j, rows_of(i), :] - mm(left3[i], right3[j], NT)

    @pl.loop(0, count)
    def _(k):
        @pl.when(k == 1)
        def _():
            each_group(lambda s: s < me, lambda c: c.wait())

        @pl.when(k > 0)
        def _():
            g[k, rows_of(k), :] = g[k, rows_of(k), :] - mm(left3[k], right3[k], NT)

        left = count - k
        tasks = jnp.where(k > 0, left * (left + 1) // 2 + left * extra - 1, 0)
        issued = []

        def beside():
            for _ in range(BESIDE):
                update(len(issued), tasks)
                issued.append(None)

        inverse_factor(g[k, rows_of(k), :], x_ref, work_ref, beside)

        @pl.loop(len(issued), jnp.maximum(tasks, len(issued)))
        def _(t):
            update(t, tasks)

        hi, lo = split(x_ref[...])
        x3 = jnp.concatenate([hi, lo, hi], axis=1)

        @pl.loop(0, (blocks + extra - k) // 2)
        def _(c):
            i = k + 1 + 2 * c
            hi, lo = split(g[k, rows_of(i, 2), :])
            done = mm(jnp.concatenate([hi, hi, lo], axis=1), x3, NT)
            g[k, rows_of(i, 2), :] = done
            hi, lo = split(done)
            for n in range(2):
                part = slice(n * size, (n + 1) * size)
                left3[i + n] = jnp.concatenate([hi[part], hi[part], lo[part]], axis=1)
                right3[i + n] = jnp.concatenate([hi[part], lo[part], hi[part]], axis=1)

    rows = out_ref.shape[0]
    for h in range(per):
        out_ref[:, h * size:(h + 1) * size] = g[me * per + h, blocks * size:blocks * size + rows, :] * scale


def factor_apply(me, order, bundles, g_arrays, shares, b_groups, size, scale):
    groups, per = len(b_groups), len(b_groups[0])
    swaps = len(g_arrays[0]) - shares
    rows = b_groups[0][0].shape[0]
    blocks = groups * per
    extra = -(-rows // size)
    most, table = task_table(blocks, per, extra)
    any_spec = pl.BlockSpec(memory_space=pl.ANY)
    smem = pl.BlockSpec(memory_space=pltpu.SMEM)
    arrays = sum(g_arrays, []) + sum(b_groups, [])
    return pl.pallas_call(
        functools.partial(factor_kernel, blocks, size, groups, bundles, shares, swaps, scale, extra, most),
        out_shape=jax.ShapeDtypeStruct((rows, per * size), F32),
        in_specs=[smem, smem, smem] + [any_spec] * len(arrays),
        out_specs=pl.BlockSpec(memory_space=pltpu.VMEM),
        scratch_shapes=[
            pltpu.VMEM((blocks, (blocks + extra + 1) * size, size), F32),
            pltpu.VMEM((blocks + extra + 1, size, 3 * size), BF16),
            pltpu.VMEM((blocks + extra + 1, size, 3 * size), BF16),
            pltpu.VMEM((size, size), F32),
            pltpu.VMEM((size, size), F32),
            pltpu.SemaphoreType.DMA((groups * per * (shares * (1 + swaps) + 1),)),
        ],
        compiler_params=pltpu.CompilerParams(vmem_limit_bytes=56 * 1024 * 1024),
        cost_estimate=pl.CostEstimate(flops=6 * 10**10, bytes_accessed=2 * 10**7, transcendentals=0),
        name="factor",
    )(me, order, table, *arrays)


def image_call(places, s_places, blocks, starts, sizes, per, inner=None):
    last = inner is not None
    rows_n, cols_n, layers = sizes
    cut, wide = blocks[0][0].shape
    cuts = len(blocks[0])
    rows_s, panel = starts[0].shape
    any_spec = pl.BlockSpec(memory_space=pl.ANY)
    smem = pl.BlockSpec(memory_space=pltpu.SMEM)
    vmem = pl.BlockSpec(memory_space=pltpu.VMEM)
    scratch = [
        pltpu.VMEM((rows_n, cuts * cut, wide), F32),
        pltpu.VMEM((rows_n * layers, rows_s, panel), F32),
        pltpu.SemaphoreType.DMA((len(blocks) * cuts + len(starts),)),
    ]
    flat = sum(blocks, [])
    if last:
        shape = [jax.ShapeDtypeStruct((cols_n, rows_s, panel // per), F32)] * (per * layers)
        spec = [any_spec] * (per * layers)
        scratch += [
            pltpu.VMEM((wide, panel), F32),
            pltpu.VMEM((rows_n, layers, rows_s, panel), F32),
            pltpu.SemaphoreType.DMA((rows_n, layers, per)),
        ]
        flops = 6 * wide * panel * cuts * cut * (rows_n + 1)
    else:
        shape, spec = jax.ShapeDtypeStruct((wide, panel), F32), vmem
        flops = 6 * wide * panel * cuts * cut * (rows_n - 1)
    return pl.pallas_call(
        functools.partial(image_kernel, sizes, cuts, per, last),
        out_shape=shape,
        in_specs=[smem, smem] + [any_spec] * (len(flat) + len(starts)) + [vmem] * last,
        out_specs=spec,
        scratch_shapes=scratch,
        compiler_params=pltpu.CompilerParams(vmem_limit_bytes=56 * 1024 * 1024),
        cost_estimate=pl.CostEstimate(flops=flops, bytes_accessed=4 * cuts * cut * wide * rows_n, transcendentals=0),
        name="image" if last else "inner",
    )(places, s_places, *flat, *starts, *([inner] if last else []))


def image_kernel(sizes, cuts, per, last, place_ref, s_place_ref, *refs):
    rows_n, cols_n, layers = sizes
    far = rows_n - 1
    hops = [0]
    for step in range(1, rows_n if last else far):
        hops += [-step, step]
    n_a, shares = len(hops) * cuts, cols_n * layers
    a_refs, s_refs, refs = refs[:n_a], refs[n_a:n_a + shares], refs[n_a + shares:]
    if last:
        outs = refs[1:1 + per * layers]
        a, s, sem, acc, o, out_sem = refs[1 + per * layers:]
    else:
        acc, a, s, sem = refs
    me, col, layer = place_ref[0], place_ref[1], place_ref[2]
    cut = a_refs[0].shape[0]
    rows_s, panel = s_refs[0].shape
    size = panel // per

    def each_block(z, act):
        for n in range(n_a):
            @pl.when(me + hops[n // cuts] == z)
            def _():
                act(pltpu.make_async_copy(
                    a_refs[n], a.at[z, pl.ds(n % cuts * cut, cut), :], sem.at[n]))

    def each_share(z, act):
        for n in range(shares):
            @pl.when(s_place_ref[n] // layers == z)
            def _():
                act(pltpu.make_async_copy(s_refs[n], s.at[s_place_ref[n]], sem.at[n_a + n]))

    def rows_of(m):
        return pl.ds(pl.multiple_of(m * rows_s, rows_s), rows_s)

    def add_product(z):
        each_block(z, lambda c: c.wait())
        each_share(z, lambda c: c.wait())

        @pl.loop(0, layers)
        def _(m):
            acc[...] += mm3(split(a[z, rows_of(m), :]), split(s[z * layers + m]), TN)

    if not last:
        acc[...] = jnp.zeros_like(acc)

        @pl.loop(0, rows_n)
        def _(step):
            z = lax.rem(me + step, rows_n)
            each_block(z, lambda c: c.start())

            @pl.when(jnp.abs(z - me) < far)
            def _():
                each_share(z, lambda c: c.start())

        @pl.loop(0, rows_n)
        def _(step):
            z = lax.rem(me + step, rows_n)

            @pl.when(jnp.abs(z - me) < far)
            def _():
                add_product(z)

        return

    def each_out(z, m, act):
        for x in range(layers):
            @pl.when(jnp.bitwise_xor(m, layer) == x)
            def _():
                for h in range(per):
                    act(pltpu.make_async_copy(
                        o.at[z, m, :, pl.ds(h * size, size)],
                        outs[x * per + h].at[jnp.bitwise_xor(z, col)], out_sem.at[z, m, h]))

    far_z = far - me
    ends = jnp.abs(far_z - me) == far

    @pl.when(ends)
    def _():
        each_block(far_z, lambda c: c.start())
        each_share(far_z, lambda c: c.start())

    @pl.loop(0, rows_n)
    def _(z):
        @pl.when(jnp.abs(z - me) < far)
        def _():
            each_block(z, lambda c: c.start())

    acc[...] = refs[0][...]

    @pl.when(ends)
    def _():
        add_product(far_z)

    inner = split(acc[...])

    @pl.loop(0, rows_n)
    def _(z):
        @pl.when(jnp.abs(z - me) < far)
        def _():
            each_block(z, lambda c: c.wait())

        @pl.loop(0, layers)
        def _(m):
            o[z, m] = mm3(split(a[z, rows_of(m), :]), inner, NN)
            each_out(z, m, lambda c: c.start())

    @pl.loop(0, rows_n)
    def _(z):
        @pl.loop(0, layers)
        def _(m):
            each_out(z, m, lambda c: c.wait())


def gram_kernel(bundle, sizes, per, place_ref, *refs):
    cols_n, layers = sizes
    shares = cols_n * layers
    n_p = (bundle[-1] + 1) * per
    p_refs, outs, (left3, right3, g, sem) = refs[:n_p], refs[n_p:n_p + layers], refs[n_p + layers:]
    rows, size = p_refs[0].shape
    width = size * per
    col, layer = place_ref[1], place_ref[2]
    for t in range(bundle[-1] + 1):
        for h in range(per):
            hi, lo = split(p_refs[t * per + h][...])
            here = pl.ds(h * size, size)
            for n, part in enumerate((hi, hi, lo)):
                left3[t, n * rows:(n + 1) * rows, here] = part
            if t in bundle:
                for n, part in enumerate((hi, lo, hi)):
                    right3[bundle.index(t), n * rows:(n + 1) * rows, here] = part
    base, first = 0, 0
    copies = []
    for i, s in enumerate(bundle):
        for t in range(s, -1, -1):
            at = base + (s - t) * width
            g[at:at + width, :] = mm(left3[t], right3[i], TN)
        n = (s + 1) * width // shares
        for x in range(layers):
            for y in range(cols_n):
                share = jnp.bitwise_xor(layer, x) * cols_n + jnp.bitwise_xor(col, y)
                start = pl.multiple_of(base + share * n, 8)
                copies.append(pltpu.make_async_copy(
                    g.at[pl.ds(start, n), :], outs[x].at[y, pl.ds(first, n), :], sem.at[len(copies)]))
                copies[-1].start()
        base += (s + 1) * width
        first += n
    for c in copies:
        c.wait()


def gram_call(place, bundle, panels, sizes):
    cols_n, layers = sizes
    per = len(panels[0])
    rows, size = panels[0][0].shape
    width = size * per
    total = sum(s + 1 for s in bundle) * width
    flat = sum(panels[:bundle[-1] + 1], [])
    vmem = pl.BlockSpec(memory_space=pltpu.VMEM)
    return pl.pallas_call(
        functools.partial(gram_kernel, bundle, sizes, per),
        out_shape=[jax.ShapeDtypeStruct((cols_n, total // (cols_n * layers), width), F32)] * layers,
        in_specs=[pl.BlockSpec(memory_space=pltpu.SMEM)] + [vmem] * len(flat),
        out_specs=[pl.BlockSpec(memory_space=pl.ANY)] * layers,
        scratch_shapes=[
            pltpu.VMEM((bundle[-1] + 1, 3 * rows, width), BF16),
            pltpu.VMEM((len(bundle), 3 * rows, width), BF16),
            pltpu.VMEM((total, width), F32),
            pltpu.SemaphoreType.DMA((len(bundle) * cols_n * layers,)),
        ],
        compiler_params=pltpu.CompilerParams(vmem_limit_bytes=48 * 1024 * 1024),
        cost_estimate=pl.CostEstimate(flops=6 * total * width * rows, bytes_accessed=4 * total * width, transcendentals=0),
        name="gram",
    )(place, *flat)


def shift_by_xor(x, axis, step):
    n = lax.axis_size(axis)
    return lax.ppermute(x, axis, [(a, a ^ step) for a in range(n)])


def own_and_others(x, axis, heavy=0):
    if heavy and lax.axis_size(axis) == 4:
        near, side = shift_by_xor(x, axis, 3 ^ heavy), shift_by_xor(x, axis, heavy)
        got = {0: x, 3 ^ heavy: near, heavy: side, 3: shift_by_xor(near, axis, heavy)}
        return [got[s] for s in range(4)]
    return [x] + [shift_by_xor(x, axis, s) for s in range(1, lax.axis_size(axis))]


def exchange_sum(parts, axis, heavy=0):
    if heavy and len(parts) == 4:
        light = 3 ^ heavy
        through = shift_by_xor(parts[3], axis, heavy)
        came = shift_by_xor(parts[heavy], axis, heavy)
        onward = parts[light] + through
        onward = shift_by_xor(onward, axis, light)
        return parts[0] + came + onward
    came = [shift_by_xor(parts[s], axis, s) for s in range(1, len(parts))]
    return sum(came, parts[0])


def chain(x, axis, direction):
    n = lax.axis_size(axis)
    pairs = [(a, a + direction) for a in range(n) if 0 <= a + direction < n]
    got = [x]
    for _ in range(n - 1):
        got.append(lax.ppermute(got[-1], axis, pairs))
    return got


def shards(wavefunction, start_block):
    sizes = rows_n, cols_n, layers = tuple(lax.axis_size(a) for a in ("row", "col", "layer"))
    row, col, layer = (lax.axis_index(a).astype(jnp.int32) for a in ("row", "col", "layer"))
    order_m = wavefunction.shape[0] * rows_n
    panel = start_block.shape[1]
    size = min(256, panel)
    per = panel // size
    place = jnp.stack([row, col, layer])

    width = wavefunction.shape[1] // layers
    own = lax.dynamic_slice_in_dim(wavefunction, layer * width, width, 1)
    chains = [(chain(cut, "row", 1), chain(cut, "row", -1)) for cut in jnp.split(own, 2)]
    blocks = [[c[0][0] for c in chains]]
    for s in range(1, rows_n):
        blocks += [[c[0][s] for c in chains], [c[1][s] for c in chains]]
    starts, s_places = [], []
    for s, part in enumerate(own_and_others(start_block, "col")):
        for t, piece in enumerate(own_and_others(part, "layer")):
            starts.append(piece)
            s_places.append((col ^ s) * layers + (layer ^ t))
    s_places = jnp.stack(s_places)
    inner = image_call(place, s_places, blocks[:-2], starts, sizes, per)
    images = image_call(place, s_places, blocks, starts, sizes, per, inner)
    panels = [[]]
    for h in range(per):
        image = exchange_sum([images[x * per + h] for x in range(layers)], "layer")
        panels[0].append(exchange_sum([image[s] for s in range(cols_n)], "col", 1 + h % 2))

    bundles = [[0, 1]] + [[s] for s in range(2, rows_n)]
    up = [(a, a + 1) for a in range(rows_n - 1)]
    g_arrays = []
    for s in range(rows_n):
        if s:
            panels.append([lax.ppermute(part, "row", up) for part in panels[-1]])
        for bundle in bundles:
            if bundle[-1] == s:
                gram = gram_call(place, bundle, panels, (cols_n, layers))
                gram = exchange_sum(gram, "layer")
                gram = [gram[y] for y in range(cols_n)]
                gram = exchange_sum(gram, "col", 1)
                pieces = own_and_others(gram, "col", 2)
                g_arrays.append(pieces + own_and_others(jnp.stack(pieces), "layer")[1:])
    places = jnp.stack([(layer ^ x) * cols_n + (col ^ s) for x in range(layers) for s in range(cols_n)])
    return factor_apply(place, places, bundles, g_arrays, cols_n, panels, size, math.sqrt(order_m))


def solution(mesh):
    placed = (P("row", "col"), P(("col", "layer"), "row"))

    return jax.shard_map(shards, mesh=mesh, in_specs=placed, out_specs=P(("col", "layer"), "row"), check_vma=False)
```

```python
import functools, math
import jax, jax.numpy as jnp
from jax import lax
from jax.experimental import pallas as pl
from jax.experimental.pallas import tpu as pltpu
from jax.sharding import PartitionSpec as P

F32, BF16 = jnp.float32, jnp.bfloat16
NN = (((1,), (0,)), ((), ()))
NT = (((1,), (1,)), ((), ()))
TN = (((0,), (0,)), ((), ()))
STEPS = 5
BESIDE = 2


def mm(a, b, dims):
    return lax.dot_general(a, b, dims, preferred_element_type=F32)


def split(x):
    high = x.astype(BF16)
    return high, (x - high.astype(F32)).astype(BF16)


def mm3(a, b, dims):
    return mm(a[0], b[0], dims) + (mm(a[0], b[1], dims) + mm(a[1], b[0], dims))


def iotas(n):
    return lax.broadcasted_iota(jnp.int32, (n, n), 0), lax.broadcasted_iota(jnp.int32, (n, n), 1)


def lower_half(x, rows, cols):
    return jnp.where(rows > cols, x, jnp.where(rows == cols, 0.5 * x, 0.0))


def inverse_factor(block, out_ref, work_ref, beside):
    n = block.shape[0]
    rows, cols = iotas(n)
    eye = (rows == cols).astype(F32)
    on_diag = block * eye
    scale_row = lax.rsqrt(jnp.sum(on_diag, axis=0, keepdims=True))
    scale_col = lax.rsqrt(jnp.sum(on_diag, axis=1, keepdims=True))
    scaled = block * scale_row * scale_col
    w = scaled
    x = eye
    for step in range(STEPS):
        half = lower_half(w - eye, rows, cols)
        hb = half.astype(BF16)
        moved = mm(hb, w.astype(BF16), NN)
        x = x - (mm(hb, x.astype(BF16), NN) if step else half)
        beside()
        w = w - moved
        w = w - mm(w.astype(BF16), hb, NT)
        beside()
    xs = split(x)
    product = mm3(xs, split(scaled), NN)
    beside()
    error = mm3(split(product), xs, NT) - eye
    beside()
    x = x - mm3(split(lower_half(error, rows, cols)), xs, NN)
    beside()
    out_ref[...] = x * scale_row
    size = jnp.sum(error * error)

    @pl.when(jnp.logical_not(size < 1e-3))
    def _():
        work_ref[...] = block
        out_ref[...] = eye

        @pl.loop(0, n)
        def _(j):
            state = work_ref[...]
            factors = out_ref[...]
            column = jnp.sum(jnp.where(cols == j, state, 0.0), axis=1, keepdims=True)
            below = lax.broadcasted_iota(jnp.int32, (n, 1), 0)
            pivot = jnp.sum(jnp.where(below == j, column, 0.0), axis=0, keepdims=True)
            multiplier = jnp.where(below > j, column / pivot, 0.0)
            work_ref[...] = state - multiplier * work_ref[pl.ds(j, 1), :]
            out_ref[...] = factors - multiplier * out_ref[pl.ds(j, 1), :]

        pivots = jnp.sum(work_ref[...] * eye, axis=1, keepdims=True)
        out_ref[...] = out_ref[...] * lax.rsqrt(pivots)


def task_table(blocks, per, extra):
    lists = []
    for count in range(per, blocks + 1, per):
        mine = []
        for j in range(count - 1, 0, -1):
            mine += [(i, j) for i in list(range(j + 1, count)) + list(range(blocks, blocks + extra))] + [(j, j)]
        lists.append(mine)
    most = max(len(mine) for mine in lists) + 1
    idle = (blocks + extra, blocks - 1)
    return most, jnp.array([mine + [idle] * (most - len(mine)) for mine in lists], jnp.int32).reshape(-1)


def factor_kernel(blocks, size, groups, bundles, shares, swaps, scale, extra, most, me_ref, order_ref, table_ref, *refs):
    per = blocks // groups
    arrays = shares + swaps
    g_refs = [refs[n * arrays:(n + 1) * arrays] for n in range(len(bundles))]
    refs = refs[len(bundles) * arrays:]
    b_refs = [refs[s * per:(s + 1) * per] for s in range(groups)]
    out_ref, g, left3, right3, x_ref, work_ref, sem = refs[groups * per:]
    tall = b_refs[0][0].shape[0]
    me = me_ref[0]
    pieces = shares * (1 + swaps)
    copies = [[] for _ in range(groups)]
    n_sem = 0
    for bundle, arrays_in in zip(bundles, g_refs):
        for t in range(pieces):
            piece = arrays_in[t] if t < shares else arrays_in[shares + t // shares - 1].at[t % shares]
            first = 0
            for (s, h), (top, at), n in segments(bundle, per):
                rows = n * size // pieces
                start = pl.multiple_of(((me - top) * per + at) * size + order_ref[t] * rows, 8)
                copies[s].append(pltpu.make_async_copy(
                    piece.at[pl.ds(first, rows), :], g.at[(me - s) * per + h, pl.ds(start, rows), :], sem.at[n_sem]))
                n_sem += 1
                first += rows
    for s in range(groups):
        for h in range(per):
            copies[s].append(pltpu.make_async_copy(
                b_refs[s][h], g.at[(me - s) * per + h, pl.ds(blocks * size, tall), :], sem.at[n_sem]))
            n_sem += 1

    def each_group(wanted, act):
        for s in range(groups):
            @pl.when(wanted(s))
            def _():
                for c in copies[s]:
                    act(c)

    each_group(lambda s: s == me, lambda c: c.start())
    each_group(lambda s: s < me, lambda c: c.start())
    each_group(lambda s: s == me, lambda c: c.wait())
    count = (me + 1) * per

    def rows_of(i, n=1):
        return pl.ds(pl.multiple_of(i * size, size), n * size)

    def update(t, limit):
        at = 2 * (me * most + jnp.where(t < limit, t, most - 1))
        i, j = table_ref[at], table_ref[at + 1]
        g[j, rows_of(i), :] = g[j, rows_of(i), :] - mm(left3[i], right3[j], NT)

    @pl.loop(0, count)
    def _(k):
        @pl.when(k == 1)
        def _():
            each_group(lambda s: s < me, lambda c: c.wait())

        @pl.when(k > 0)
        def _():
            g[k, rows_of(k), :] = g[k, rows_of(k), :] - mm(left3[k], right3[k], NT)

        left = count - k
        tasks = jnp.where(k > 0, left * (left + 1) // 2 + left * extra - 1, 0)
        issued = []

        def beside():
            for _ in range(BESIDE):
                update(len(issued), tasks)
                issued.append(None)

        inverse_factor(g[k, rows_of(k), :], x_ref, work_ref, beside)

        @pl.loop(len(issued), jnp.maximum(tasks, len(issued)))
        def _(t):
            update(t, tasks)

        hi, lo = split(x_ref[...])
        x3 = jnp.concatenate([hi, lo, hi], axis=1)

        @pl.loop(0, (blocks + extra - k) // 2)
        def _(c):
            i = k + 1 + 2 * c
            hi, lo = split(g[k, rows_of(i, 2), :])
            done = mm(jnp.concatenate([hi, hi, lo], axis=1), x3, NT)
            g[k, rows_of(i, 2), :] = done
            hi, lo = split(done)
            for n in range(2):
                part = slice(n * size, (n + 1) * size)
                left3[i + n] = jnp.concatenate([hi[part], hi[part], lo[part]], axis=1)
                right3[i + n] = jnp.concatenate([hi[part], lo[part], hi[part]], axis=1)

    rows = out_ref.shape[0]
    for h in range(per):
        out_ref[:, h * size:(h + 1) * size] = g[me * per + h, blocks * size:blocks * size + rows, :] * scale


def factor_apply(me, order, bundles, g_arrays, shares, b_groups, size, scale):
    groups, per = len(b_groups), len(b_groups[0])
    swaps = len(g_arrays[0]) - shares
    rows = b_groups[0][0].shape[0]
    blocks = groups * per
    extra = -(-rows // size)
    most, table = task_table(blocks, per, extra)
    any_spec = pl.BlockSpec(memory_space=pl.ANY)
    smem = pl.BlockSpec(memory_space=pltpu.SMEM)
    arrays = sum(g_arrays, []) + sum(b_groups, [])
    return pl.pallas_call(
        functools.partial(factor_kernel, blocks, size, groups, bundles, shares, swaps, scale, extra, most),
        out_shape=jax.ShapeDtypeStruct((rows, per * size), F32),
        in_specs=[smem, smem, smem] + [any_spec] * len(arrays),
        out_specs=pl.BlockSpec(memory_space=pltpu.VMEM),
        scratch_shapes=[
            pltpu.VMEM((blocks, (blocks + extra + 1) * size, size), F32),
            pltpu.VMEM((blocks + extra + 1, size, 3 * size), BF16),
            pltpu.VMEM((blocks + extra + 1, size, 3 * size), BF16),
            pltpu.VMEM((size, size), F32),
            pltpu.VMEM((size, size), F32),
            pltpu.SemaphoreType.DMA((
                sum(len(segments(b, per)) for b in bundles) * shares * (1 + swaps) + groups * per,)),
        ],
        compiler_params=pltpu.CompilerParams(vmem_limit_bytes=56 * 1024 * 1024),
        cost_estimate=pl.CostEstimate(flops=6 * 10**10, bytes_accessed=2 * 10**7, transcendentals=0),
        name="factor",
    )(me, order, table, *arrays)


def image_call(places, s_places, blocks, starts, sizes, per, inner=None):
    last = inner is not None
    rows_n, cols_n, layers = sizes
    cut, wide = blocks[0][0].shape
    cuts = len(blocks[0])
    rows_s, panel = starts[0].shape
    any_spec = pl.BlockSpec(memory_space=pl.ANY)
    smem = pl.BlockSpec(memory_space=pltpu.SMEM)
    vmem = pl.BlockSpec(memory_space=pltpu.VMEM)
    scratch = [
        pltpu.VMEM((rows_n, cuts * cut, wide), F32),
        pltpu.VMEM((rows_n * layers, rows_s, panel), F32),
        pltpu.SemaphoreType.DMA((len(blocks) * cuts + len(starts),)),
    ]
    flat = sum(blocks, [])
    if last:
        shape = [jax.ShapeDtypeStruct((cols_n, rows_s, panel // per), F32)] * (per * layers)
        spec = [any_spec] * (per * layers)
        scratch += [
            pltpu.VMEM((wide, panel), F32),
            pltpu.VMEM((rows_n, layers, rows_s, panel), F32),
            pltpu.SemaphoreType.DMA((rows_n, layers, per)),
        ]
        flops = 6 * wide * panel * cuts * cut * (rows_n + 1)
    else:
        shape, spec = jax.ShapeDtypeStruct((wide, panel), F32), vmem
        flops = 6 * wide * panel * cuts * cut * (rows_n - 1)
    return pl.pallas_call(
        functools.partial(image_kernel, sizes, cuts, per, last),
        out_shape=shape,
        in_specs=[smem, smem] + [any_spec] * (len(flat) + len(starts)) + [vmem] * last,
        out_specs=spec,
        scratch_shapes=scratch,
        compiler_params=pltpu.CompilerParams(vmem_limit_bytes=56 * 1024 * 1024),
        cost_estimate=pl.CostEstimate(flops=flops, bytes_accessed=4 * cuts * cut * wide * rows_n, transcendentals=0),
        name="image" if last else "inner",
    )(places, s_places, *flat, *starts, *([inner] if last else []))


def image_kernel(sizes, cuts, per, last, place_ref, s_place_ref, *refs):
    rows_n, cols_n, layers = sizes
    far = rows_n - 1
    hops = [0]
    for step in range(1, rows_n if last else far):
        hops += [-step, step]
    n_a, shares = len(hops) * cuts, cols_n * layers
    a_refs, s_refs, refs = refs[:n_a], refs[n_a:n_a + shares], refs[n_a + shares:]
    if last:
        outs = refs[1:1 + per * layers]
        a, s, sem, acc, o, out_sem = refs[1 + per * layers:]
    else:
        acc, a, s, sem = refs
    me, col, layer = place_ref[0], place_ref[1], place_ref[2]
    cut = a_refs[0].shape[0]
    rows_s, panel = s_refs[0].shape
    size = panel // per

    def each_block(z, act):
        for n in range(n_a):
            @pl.when(me + hops[n // cuts] == z)
            def _():
                act(pltpu.make_async_copy(
                    a_refs[n], a.at[z, pl.ds(n % cuts * cut, cut), :], sem.at[n]))

    def each_share(z, act):
        for n in range(shares):
            @pl.when(s_place_ref[n] // layers == z)
            def _():
                act(pltpu.make_async_copy(s_refs[n], s.at[s_place_ref[n]], sem.at[n_a + n]))

    def rows_of(m):
        return pl.ds(pl.multiple_of(m * rows_s, rows_s), rows_s)

    def add_product(z):
        each_block(z, lambda c: c.wait())
        each_share(z, lambda c: c.wait())

        @pl.loop(0, layers)
        def _(m):
            acc[...] += mm3(split(a[z, rows_of(m), :]), split(s[z * layers + m]), TN)

    if not last:
        acc[...] = jnp.zeros_like(acc)

        @pl.loop(0, rows_n)
        def _(step):
            z = lax.rem(me + step, rows_n)
            each_block(z, lambda c: c.start())

            @pl.when(jnp.abs(z - me) < far)
            def _():
                each_share(z, lambda c: c.start())

        @pl.loop(0, rows_n)
        def _(step):
            z = lax.rem(me + step, rows_n)

            @pl.when(jnp.abs(z - me) < far)
            def _():
                add_product(z)

        return

    def each_out(z, m, act):
        for x in range(layers):
            @pl.when(jnp.bitwise_xor(m, layer) == x)
            def _():
                for h in range(per):
                    act(pltpu.make_async_copy(
                        o.at[z, m, :, pl.ds(h * size, size)],
                        outs[x * per + h].at[jnp.bitwise_xor(z, col)], out_sem.at[z, m, h]))

    far_z = far - me
    ends = jnp.abs(far_z - me) == far

    @pl.when(ends)
    def _():
        each_block(far_z, lambda c: c.start())
        each_share(far_z, lambda c: c.start())

    @pl.loop(0, rows_n)
    def _(z):
        @pl.when(jnp.abs(z - me) < far)
        def _():
            each_block(z, lambda c: c.start())

    acc[...] = refs[0][...]

    @pl.when(ends)
    def _():
        add_product(far_z)

    inner = split(acc[...])

    @pl.loop(0, rows_n)
    def _(z):
        @pl.when(jnp.abs(z - me) < far)
        def _():
            each_block(z, lambda c: c.wait())

        @pl.loop(0, layers)
        def _(m):
            o[z, m] = mm3(split(a[z, rows_of(m), :]), inner, NN)
            each_out(z, m, lambda c: c.start())

    @pl.loop(0, rows_n)
    def _(z):
        @pl.loop(0, layers)
        def _(m):
            each_out(z, m, lambda c: c.wait())


def segments(bundle, per):
    runs = []
    for s, h in bundle:
        runs += [((s, before), (s, h), 1) for before in range(h)]
        if h == per - 1:
            runs.append(((s, h), (s, h), 1 + s * per))
        else:
            runs.append(((s, h), (s, h), 1))
            if s:
                runs.append(((s, h), (s - 1, 0), s * per))
    return runs


def gram_kernel(bundle, known, sizes, per, place_ref, *refs):
    cols_n, layers = sizes
    shares = cols_n * layers
    top = max(s for s, _ in known)
    p_refs, outs, (left3, right3, g, sem) = refs[:len(known)], refs[len(known):len(known) + layers], refs[len(known) + layers:]
    rows, size = p_refs[0].shape
    col, layer = place_ref[1], place_ref[2]
    runs = segments(bundle, per)
    rights = sorted(set(run[0] for run in runs))

    def at(t, h):
        return (top - t) * per + h

    for n, (t, h) in enumerate(known):
        hi, lo = split(p_refs[n][...])
        for m, part in enumerate((hi, hi, lo)):
            left3[at(t, h), m * rows:(m + 1) * rows, :] = part
        if (t, h) in rights:
            for m, part in enumerate((hi, lo, hi)):
                right3[rights.index((t, h)), m * rows:(m + 1) * rows, :] = part
    base, first = 0, 0
    copies = []
    for column, row, count in runs:
        right, start = rights.index(column), at(*row)

        together = count if len(bundle) == 1 else min(4, count)
        if together == count:
            for n in range(count):
                g[base + n * size:base + (n + 1) * size, :] = mm(left3[start + n], right3[right], TN)
        else:
            @pl.loop(0, -(-count // together))
            def _(step):
                for k in range(together):
                    n = jnp.minimum(step * together + k, count - 1)
                    g[pl.ds(pl.multiple_of(base + n * size, size), size), :] = mm(left3[start + n], right3[right], TN)

        n = count * size // shares
        for x in range(layers):
            for y in range(cols_n):
                share = jnp.bitwise_xor(layer, x) * cols_n + jnp.bitwise_xor(col, y)
                start = pl.multiple_of(base + share * n, 8)
                copies.append(pltpu.make_async_copy(
                    g.at[pl.ds(start, n), :], outs[x].at[y, pl.ds(first, n), :], sem.at[len(copies)]))
                copies[-1].start()
        base += count * size
        first += n
    for c in copies:
        c.wait()


def gram_call(place, bundle, panels, sizes):
    cols_n, layers = sizes
    per = len(panels[0])
    known = [(t, h) for t in range(len(panels)) for h in range(per) if (t, h) <= bundle[-1]]
    flat = [panels[t][h] for t, h in known]
    rows, size = flat[0].shape
    runs = segments(bundle, per)
    total = sum(run[2] for run in runs) * size
    vmem = pl.BlockSpec(memory_space=pltpu.VMEM)
    return pl.pallas_call(
        functools.partial(gram_kernel, bundle, known, sizes, per),
        out_shape=[jax.ShapeDtypeStruct((cols_n, total // (cols_n * layers), size), F32)] * layers,
        in_specs=[pl.BlockSpec(memory_space=pltpu.SMEM)] + [vmem] * len(flat),
        out_specs=[pl.BlockSpec(memory_space=pl.ANY)] * layers,
        scratch_shapes=[
            pltpu.VMEM(((bundle[-1][0] + 1) * per, 3 * rows, size), BF16),
            pltpu.VMEM((len(set(run[0] for run in runs)), 3 * rows, size), BF16),
            pltpu.VMEM((total, size), F32),
            pltpu.SemaphoreType.DMA((len(runs) * cols_n * layers,)),
        ],
        compiler_params=pltpu.CompilerParams(vmem_limit_bytes=48 * 1024 * 1024),
        cost_estimate=pl.CostEstimate(flops=6 * total * size * rows, bytes_accessed=4 * total * size, transcendentals=0),
        name="gram",
    )(place, *flat)


def shift_by_xor(x, axis, step):
    n = lax.axis_size(axis)
    return lax.ppermute(x, axis, [(a, a ^ step) for a in range(n)])


def own_and_others(x, axis, heavy=0):
    if heavy and lax.axis_size(axis) == 4:
        near, side = shift_by_xor(x, axis, 3 ^ heavy), shift_by_xor(x, axis, heavy)
        got = {0: x, 3 ^ heavy: near, heavy: side, 3: shift_by_xor(near, axis, heavy)}
        return [got[s] for s in range(4)]
    return [x] + [shift_by_xor(x, axis, s) for s in range(1, lax.axis_size(axis))]


def exchange_sum(parts, axis, heavy=0):
    if heavy and len(parts) == 4:
        light = 3 ^ heavy
        through = shift_by_xor(parts[3], axis, heavy)
        came = shift_by_xor(parts[heavy], axis, heavy)
        onward = parts[light] + through
        onward = shift_by_xor(onward, axis, light)
        return parts[0] + came + onward
    came = [shift_by_xor(parts[s], axis, s) for s in range(1, len(parts))]
    return sum(came, parts[0])


def chain(x, axis, direction):
    n = lax.axis_size(axis)
    pairs = [(a, a + direction) for a in range(n) if 0 <= a + direction < n]
    got = [x]
    for _ in range(n - 1):
        got.append(lax.ppermute(got[-1], axis, pairs))
    return got


def shards(wavefunction, start_block):
    sizes = rows_n, cols_n, layers = tuple(lax.axis_size(a) for a in ("row", "col", "layer"))
    row, col, layer = (lax.axis_index(a).astype(jnp.int32) for a in ("row", "col", "layer"))
    order_m = wavefunction.shape[0] * rows_n
    panel = start_block.shape[1]
    size = min(256, panel)
    per = panel // size
    place = jnp.stack([row, col, layer])

    width = wavefunction.shape[1] // layers
    own = lax.dynamic_slice_in_dim(wavefunction, layer * width, width, 1)
    chains = [(chain(cut, "row", 1), chain(cut, "row", -1)) for cut in jnp.split(own, 2)]
    blocks = [[c[0][0] for c in chains]]
    for s in range(1, rows_n):
        blocks += [[c[0][s] for c in chains], [c[1][s] for c in chains]]
    starts, s_places = [], []
    for s, part in enumerate(own_and_others(start_block, "col")):
        for t, piece in enumerate(own_and_others(part, "layer")):
            starts.append(piece)
            s_places.append((col ^ s) * layers + (layer ^ t))
    s_places = jnp.stack(s_places)
    inner = image_call(place, s_places, blocks[:-2], starts, sizes, per)
    images = image_call(place, s_places, blocks, starts, sizes, per, inner)
    panels = [[]]
    for h in range(per):
        image = exchange_sum([images[x * per + h] for x in range(layers)], "layer")
        panels[0].append(exchange_sum([image[s] for s in range(cols_n)], "col", 1 + h % 2))

    bundles = all_bundles(rows_n, per)
    up = [(a, a + 1) for a in range(rows_n - 1)]
    g_arrays = []
    for n, bundle in enumerate(bundles):
        s = bundle[-1][0]
        if s == len(panels):
            panels.append([])
            for h in range(per):
                panels[-1].append(lax.ppermute(panels[-2][h], "row", up))
        gram = gram_call(place, bundle, panels, (cols_n, layers))
        gram = exchange_sum(gram, "layer")
        gram = [gram[y] for y in range(cols_n)]
        direct = n >= rows_n - 2
        gram = exchange_sum(gram, "col", 0 if direct else 1)
        pieces = own_and_others(gram, "col", 0 if direct else 2)
        stack = jnp.stack(pieces)
        g_arrays.append(pieces + own_and_others(stack, "layer")[1:])
    places = jnp.stack([(layer ^ x) * cols_n + (col ^ s) for x in range(layers) for s in range(cols_n)])
    return factor_apply(place, places, bundles, g_arrays, cols_n, panels, size, math.sqrt(order_m))


def all_bundles(rows_n, per):
    whole = [[(s, h) for h in range(per)] for s in range(rows_n - 1)]
    return whole + [[(rows_n - 1, h)] for h in range(per)]


def solution(mesh):
    placed = (P("row", "col"), P(("col", "layer"), "row"))

    return jax.shard_map(shards, mesh=mesh, in_specs=placed, out_specs=P(("col", "layer"), "row"), check_vma=False)
```

```python
import functools, math
import jax, jax.numpy as jnp
from jax import lax
from jax.experimental import pallas as pl
from jax.experimental.pallas import tpu as pltpu
from jax.sharding import PartitionSpec as P

F32, BF16 = jnp.float32, jnp.bfloat16
NN = (((1,), (0,)), ((), ()))
NT = (((1,), (1,)), ((), ()))
TN = (((0,), (0,)), ((), ()))
STEPS = 5
BESIDE = 2


def mm(a, b, dims):
    return lax.dot_general(a, b, dims, preferred_element_type=F32)


def split(x):
    high = x.astype(BF16)
    return high, (x - high.astype(F32)).astype(BF16)


def mm3(a, b, dims):
    return mm(a[0], b[0], dims) + (mm(a[0], b[1], dims) + mm(a[1], b[0], dims))


def iotas(n):
    return lax.broadcasted_iota(jnp.int32, (n, n), 0), lax.broadcasted_iota(jnp.int32, (n, n), 1)


def lower_half(x, rows, cols):
    return jnp.where(rows > cols, x, jnp.where(rows == cols, 0.5 * x, 0.0))


def inverse_factor(block, out_ref, work_ref, beside):
    n = block.shape[0]
    rows, cols = iotas(n)
    eye = (rows == cols).astype(F32)
    on_diag = block * eye
    scale_row = lax.rsqrt(jnp.sum(on_diag, axis=0, keepdims=True))
    scale_col = lax.rsqrt(jnp.sum(on_diag, axis=1, keepdims=True))
    scaled = block * scale_row * scale_col
    w = scaled
    x = eye
    for step in range(STEPS):
        half = lower_half(w - eye, rows, cols)
        hb = half.astype(BF16)
        moved = mm(hb, w.astype(BF16), NN)
        x = x - (mm(hb, x.astype(BF16), NN) if step else half)
        beside()
        w = w - moved
        w = w - mm(w.astype(BF16), hb, NT)
        beside()
    xs = split(x)
    product = mm3(xs, split(scaled), NN)
    beside()
    error = mm3(split(product), xs, NT) - eye
    beside()
    x = x - mm3(split(lower_half(error, rows, cols)), xs, NN)
    beside()
    out_ref[...] = x * scale_row
    size = jnp.sum(error * error)

    @pl.when(jnp.logical_not(size < 1e-3))
    def _():
        work_ref[...] = block
        out_ref[...] = eye

        @pl.loop(0, n)
        def _(j):
            state = work_ref[...]
            factors = out_ref[...]
            column = jnp.sum(jnp.where(cols == j, state, 0.0), axis=1, keepdims=True)
            below = lax.broadcasted_iota(jnp.int32, (n, 1), 0)
            pivot = jnp.sum(jnp.where(below == j, column, 0.0), axis=0, keepdims=True)
            multiplier = jnp.where(below > j, column / pivot, 0.0)
            work_ref[...] = state - multiplier * work_ref[pl.ds(j, 1), :]
            out_ref[...] = factors - multiplier * out_ref[pl.ds(j, 1), :]

        pivots = jnp.sum(work_ref[...] * eye, axis=1, keepdims=True)
        out_ref[...] = out_ref[...] * lax.rsqrt(pivots)


def task_table(blocks, per, extra):
    lists = []
    for count in range(per, blocks + 1, per):
        mine = []
        for j in range(count - 1, 0, -1):
            mine += [(i, j) for i in list(range(j + 1, count)) + list(range(blocks, blocks + extra))] + [(j, j)]
        lists.append(mine)
    most = max(len(mine) for mine in lists) + 1
    idle = (blocks + extra, blocks - 1)
    return most, jnp.array([mine + [idle] * (most - len(mine)) for mine in lists], jnp.int32).reshape(-1)


def factor_kernel(blocks, size, groups, bundles, shares, swaps, scale, extra, most, me_ref, order_ref, table_ref, *refs):
    per = blocks // groups
    arrays = shares + swaps
    g_refs = [refs[n * arrays:(n + 1) * arrays] for n in range(len(bundles))]
    refs = refs[len(bundles) * arrays:]
    b_refs = [refs[s * per:(s + 1) * per] for s in range(groups)]
    out_ref, g, left3, right3, x_ref, work_ref, sem = refs[groups * per:]
    tall = b_refs[0][0].shape[0]
    me = me_ref[0]
    pieces = shares * (1 + swaps)
    copies = [[] for _ in range(groups)]
    n_sem = 0
    for bundle, arrays_in in zip(bundles, g_refs):
        for t in range(pieces):
            piece = arrays_in[t] if t < shares else arrays_in[shares + t // shares - 1].at[t % shares]
            first = 0
            for (s, h), (top, at), n in segments(bundle, per):
                rows = n * size // pieces
                start = pl.multiple_of(((me - top) * per + at) * size + order_ref[t] * rows, 8)
                copies[s].append(pltpu.make_async_copy(
                    piece.at[pl.ds(first, rows), :], g.at[(me - s) * per + h, pl.ds(start, rows), :], sem.at[n_sem]))
                n_sem += 1
                first += rows
    for s in range(groups):
        for h in range(per):
            copies[s].append(pltpu.make_async_copy(
                b_refs[s][h], g.at[(me - s) * per + h, pl.ds(blocks * size, tall), :], sem.at[n_sem]))
            n_sem += 1

    def each_group(wanted, act):
        for s in range(groups):
            @pl.when(wanted(s))
            def _():
                for c in copies[s]:
                    act(c)

    each_group(lambda s: s == me, lambda c: c.start())
    each_group(lambda s: s < me, lambda c: c.start())
    each_group(lambda s: s == me, lambda c: c.wait())
    count = (me + 1) * per

    def rows_of(i, n=1):
        return pl.ds(pl.multiple_of(i * size, size), n * size)

    def update(t, limit):
        at = 2 * (me * most + jnp.where(t < limit, t, most - 1))
        i, j = table_ref[at], table_ref[at + 1]
        g[j, rows_of(i), :] = g[j, rows_of(i), :] - mm(left3[i], right3[j], NT)

    @pl.loop(0, count)
    def _(k):
        @pl.when(k == 1)
        def _():
            each_group(lambda s: s < me, lambda c: c.wait())

        @pl.when(k > 0)
        def _():
            g[k, rows_of(k), :] = g[k, rows_of(k), :] - mm(left3[k], right3[k], NT)

        left = count - k
        tasks = jnp.where(k > 0, left * (left + 1) // 2 + left * extra - 1, 0)
        issued = []

        def beside():
            for _ in range(BESIDE):
                update(len(issued), tasks)
                issued.append(None)

        inverse_factor(g[k, rows_of(k), :], x_ref, work_ref, beside)

        @pl.loop(len(issued), jnp.maximum(tasks, len(issued)))
        def _(t):
            update(t, tasks)

        hi, lo = split(x_ref[...])
        x3 = jnp.concatenate([hi, lo, hi], axis=1)

        @pl.loop(0, (blocks + extra - k) // 2)
        def _(c):
            i = k + 1 + 2 * c
            hi, lo = split(g[k, rows_of(i, 2), :])
            done = mm(jnp.concatenate([hi, hi, lo], axis=1), x3, NT)
            g[k, rows_of(i, 2), :] = done
            hi, lo = split(done)
            for n in range(2):
                part = slice(n * size, (n + 1) * size)
                left3[i + n] = jnp.concatenate([hi[part], hi[part], lo[part]], axis=1)
                right3[i + n] = jnp.concatenate([hi[part], lo[part], hi[part]], axis=1)

    rows = out_ref.shape[0]
    for h in range(per):
        out_ref[:, h * size:(h + 1) * size] = g[me * per + h, blocks * size:blocks * size + rows, :] * scale


def factor_apply(me, order, bundles, g_arrays, shares, b_groups, size, scale):
    groups, per = len(b_groups), len(b_groups[0])
    swaps = len(g_arrays[0]) - shares
    rows = b_groups[0][0].shape[0]
    blocks = groups * per
    extra = -(-rows // size)
    most, table = task_table(blocks, per, extra)
    any_spec = pl.BlockSpec(memory_space=pl.ANY)
    smem = pl.BlockSpec(memory_space=pltpu.SMEM)
    arrays = sum(g_arrays, []) + sum(b_groups, [])
    return pl.pallas_call(
        functools.partial(factor_kernel, blocks, size, groups, bundles, shares, swaps, scale, extra, most),
        out_shape=jax.ShapeDtypeStruct((rows, per * size), F32),
        in_specs=[smem, smem, smem] + [any_spec] * len(arrays),
        out_specs=pl.BlockSpec(memory_space=pltpu.VMEM),
        scratch_shapes=[
            pltpu.VMEM((blocks, (blocks + extra + 1) * size, size), F32),
            pltpu.VMEM((blocks + extra + 1, size, 3 * size), BF16),
            pltpu.VMEM((blocks + extra + 1, size, 3 * size), BF16),
            pltpu.VMEM((size, size), F32),
            pltpu.VMEM((size, size), F32),
            pltpu.SemaphoreType.DMA((
                sum(len(segments(b, per)) for b in bundles) * shares * (1 + swaps) + groups * per,)),
        ],
        compiler_params=pltpu.CompilerParams(vmem_limit_bytes=56 * 1024 * 1024),
        cost_estimate=pl.CostEstimate(flops=6 * 10**10, bytes_accessed=2 * 10**7, transcendentals=0),
        name="factor",
    )(me, order, table, *arrays)


def image_call(places, s_places, blocks, starts, sizes, per, inner=None):
    last = inner is not None
    rows_n, cols_n, layers = sizes
    cut, wide = blocks[0][0].shape
    cuts = len(blocks[0])
    rows_s, panel = starts[0].shape
    any_spec = pl.BlockSpec(memory_space=pl.ANY)
    smem = pl.BlockSpec(memory_space=pltpu.SMEM)
    vmem = pl.BlockSpec(memory_space=pltpu.VMEM)
    scratch = [
        pltpu.VMEM((rows_n, cuts * cut, wide), F32),
        pltpu.VMEM((rows_n * layers, rows_s, panel), F32),
        pltpu.SemaphoreType.DMA((len(blocks) * cuts + len(starts),)),
    ]
    flat = sum(blocks, [])
    if last:
        shape = [jax.ShapeDtypeStruct((cols_n, rows_s, panel // per), F32)] * (per * layers)
        spec = [any_spec] * (per * layers)
        scratch += [
            pltpu.VMEM((wide, panel), F32),
            pltpu.VMEM((rows_n, layers, rows_s, panel), F32),
            pltpu.SemaphoreType.DMA((rows_n, layers, per)),
        ]
        flops = 6 * wide * panel * cuts * cut * (rows_n + 1)
    else:
        shape, spec = jax.ShapeDtypeStruct((wide, panel), F32), vmem
        flops = 6 * wide * panel * cuts * cut * (rows_n - 1)
    return pl.pallas_call(
        functools.partial(image_kernel, sizes, cuts, per, last),
        out_shape=shape,
        in_specs=[smem, smem] + [any_spec] * (len(flat) + len(starts)) + [vmem] * last,
        out_specs=spec,
        scratch_shapes=scratch,
        compiler_params=pltpu.CompilerParams(vmem_limit_bytes=56 * 1024 * 1024),
        cost_estimate=pl.CostEstimate(flops=flops, bytes_accessed=4 * cuts * cut * wide * rows_n, transcendentals=0),
        name="image" if last else "inner",
    )(places, s_places, *flat, *starts, *([inner] if last else []))


def image_kernel(sizes, cuts, per, last, place_ref, s_place_ref, *refs):
    rows_n, cols_n, layers = sizes
    far = rows_n - 1
    hops = [0]
    for step in range(1, rows_n if last else far):
        hops += [-step, step]
    n_a, shares = len(hops) * cuts, cols_n * layers
    a_refs, s_refs, refs = refs[:n_a], refs[n_a:n_a + shares], refs[n_a + shares:]
    if last:
        outs = refs[1:1 + per * layers]
        a, s, sem, acc, o, out_sem = refs[1 + per * layers:]
    else:
        acc, a, s, sem = refs
    me, col, layer = place_ref[0], place_ref[1], place_ref[2]
    cut = a_refs[0].shape[0]
    rows_s, panel = s_refs[0].shape
    size = panel // per

    def each_block(z, act):
        for n in range(n_a):
            @pl.when(me + hops[n // cuts] == z)
            def _():
                act(pltpu.make_async_copy(
                    a_refs[n], a.at[z, pl.ds(n % cuts * cut, cut), :], sem.at[n]))

    def each_share(z, act):
        for n in range(shares):
            @pl.when(s_place_ref[n] // layers == z)
            def _():
                act(pltpu.make_async_copy(s_refs[n], s.at[s_place_ref[n]], sem.at[n_a + n]))

    def rows_of(m):
        return pl.ds(pl.multiple_of(m * rows_s, rows_s), rows_s)

    def add_product(z):
        each_block(z, lambda c: c.wait())
        each_share(z, lambda c: c.wait())

        @pl.loop(0, layers)
        def _(m):
            acc[...] += mm3(split(a[z, rows_of(m), :]), split(s[z * layers + m]), TN)

    if not last:
        acc[...] = jnp.zeros_like(acc)

        @pl.loop(0, rows_n)
        def _(step):
            z = lax.rem(me + step, rows_n)
            each_block(z, lambda c: c.start())

            @pl.when(jnp.abs(z - me) < far)
            def _():
                each_share(z, lambda c: c.start())

        @pl.loop(0, rows_n)
        def _(step):
            z = lax.rem(me + step, rows_n)

            @pl.when(jnp.abs(z - me) < far)
            def _():
                add_product(z)

        return

    def each_out(z, m, act):
        for x in range(layers):
            @pl.when(jnp.bitwise_xor(m, layer) == x)
            def _():
                for h in range(per):
                    act(pltpu.make_async_copy(
                        o.at[z, m, :, pl.ds(h * size, size)],
                        outs[x * per + h].at[jnp.bitwise_xor(z, col)], out_sem.at[z, m, h]))

    far_z = far - me
    ends = jnp.abs(far_z - me) == far

    @pl.when(ends)
    def _():
        each_block(far_z, lambda c: c.start())
        each_share(far_z, lambda c: c.start())

    @pl.loop(0, rows_n)
    def _(z):
        @pl.when(jnp.abs(z - me) < far)
        def _():
            each_block(z, lambda c: c.start())

    acc[...] = refs[0][...]

    @pl.when(ends)
    def _():
        add_product(far_z)

    inner = split(acc[...])

    @pl.loop(0, rows_n)
    def _(z):
        @pl.when(jnp.abs(z - me) < far)
        def _():
            each_block(z, lambda c: c.wait())

        @pl.loop(0, layers)
        def _(m):
            o[z, m] = mm3(split(a[z, rows_of(m), :]), inner, NN)
            each_out(z, m, lambda c: c.start())

    @pl.loop(0, rows_n)
    def _(z):
        @pl.loop(0, layers)
        def _(m):
            each_out(z, m, lambda c: c.wait())


def segments(bundle, per):
    runs = []
    for s, h in bundle:
        runs += [((s, before), (s, h), 1) for before in range(h)]
        if h == per - 1:
            runs.append(((s, h), (s, h), 1 + s * per))
        else:
            runs.append(((s, h), (s, h), 1))
            if s:
                runs.append(((s, h), (s - 1, 0), s * per))
    return runs


def gram_kernel(bundle, known, sizes, per, place_ref, *refs):
    cols_n, layers = sizes
    shares = cols_n * layers
    top = max(s for s, _ in known)
    p_refs, outs, (left3, right3, g, sem) = refs[:len(known)], refs[len(known):len(known) + layers], refs[len(known) + layers:]
    rows, size = p_refs[0].shape
    col, layer = place_ref[1], place_ref[2]
    runs = segments(bundle, per)
    rights = sorted(set(run[0] for run in runs))

    def at(t, h):
        return (top - t) * per + h

    for n, (t, h) in enumerate(known):
        hi, lo = split(p_refs[n][...])
        for m, part in enumerate((hi, hi, lo)):
            left3[at(t, h), m * rows:(m + 1) * rows, :] = part
        if (t, h) in rights:
            for m, part in enumerate((hi, lo, hi)):
                right3[rights.index((t, h)), m * rows:(m + 1) * rows, :] = part
    base, first = 0, 0
    copies = []
    for column, row, count in runs:
        right, start = rights.index(column), at(*row)

        together = count if len(bundle) == 1 else min(4, count)
        if together == count:
            for n in range(count):
                g[base + n * size:base + (n + 1) * size, :] = mm(left3[start + n], right3[right], TN)
        else:
            @pl.loop(0, -(-count // together))
            def _(step):
                for k in range(together):
                    n = jnp.minimum(step * together + k, count - 1)
                    g[pl.ds(pl.multiple_of(base + n * size, size), size), :] = mm(left3[start + n], right3[right], TN)

        n = count * size // shares
        for x in range(layers):
            for y in range(cols_n):
                share = jnp.bitwise_xor(layer, x) * cols_n + jnp.bitwise_xor(col, y)
                start = pl.multiple_of(base + share * n, 8)
                copies.append(pltpu.make_async_copy(
                    g.at[pl.ds(start, n), :], outs[x].at[y, pl.ds(first, n), :], sem.at[len(copies)]))
                copies[-1].start()
        base += count * size
        first += n
    for c in copies:
        c.wait()


def gram_call(place, bundle, panels, sizes):
    cols_n, layers = sizes
    per = len(panels[0])
    known = [(t, h) for t in range(len(panels)) for h in range(per) if (t, h) <= bundle[-1]]
    flat = [panels[t][h] for t, h in known]
    rows, size = flat[0].shape
    runs = segments(bundle, per)
    total = sum(run[2] for run in runs) * size
    vmem = pl.BlockSpec(memory_space=pltpu.VMEM)
    return pl.pallas_call(
        functools.partial(gram_kernel, bundle, known, sizes, per),
        out_shape=[jax.ShapeDtypeStruct((cols_n, total // (cols_n * layers), size), F32)] * layers,
        in_specs=[pl.BlockSpec(memory_space=pltpu.SMEM)] + [vmem] * len(flat),
        out_specs=[pl.BlockSpec(memory_space=pl.ANY)] * layers,
        scratch_shapes=[
            pltpu.VMEM(((bundle[-1][0] + 1) * per, 3 * rows, size), BF16),
            pltpu.VMEM((len(set(run[0] for run in runs)), 3 * rows, size), BF16),
            pltpu.VMEM((total, size), F32),
            pltpu.SemaphoreType.DMA((len(runs) * cols_n * layers,)),
        ],
        compiler_params=pltpu.CompilerParams(vmem_limit_bytes=48 * 1024 * 1024),
        cost_estimate=pl.CostEstimate(flops=6 * total * size * rows, bytes_accessed=4 * total * size, transcendentals=0),
        name="gram",
    )(place, *flat)


def shift_by_xor(x, axis, step):
    n = lax.axis_size(axis)
    return lax.ppermute(x, axis, [(a, a ^ step) for a in range(n)])


def own_and_others(x, axis, heavy=0):
    if heavy and lax.axis_size(axis) == 4:
        near, side = shift_by_xor(x, axis, 3 ^ heavy), shift_by_xor(x, axis, heavy)
        got = {0: x, 3 ^ heavy: near, heavy: side, 3: shift_by_xor(near, axis, heavy)}
        return [got[s] for s in range(4)]
    return [x] + [shift_by_xor(x, axis, s) for s in range(1, lax.axis_size(axis))]


def exchange_sum(parts, axis, heavy=0):
    if heavy and len(parts) == 4:
        light = 3 ^ heavy
        through = shift_by_xor(parts[3], axis, heavy)
        came = shift_by_xor(parts[heavy], axis, heavy)
        onward = parts[light] + through
        onward = shift_by_xor(onward, axis, light)
        return parts[0] + came + onward
    came = [shift_by_xor(parts[s], axis, s) for s in range(1, len(parts))]
    return sum(came, parts[0])


def chain(x, axis, direction):
    n = lax.axis_size(axis)
    pairs = [(a, a + direction) for a in range(n) if 0 <= a + direction < n]
    got = [x]
    for _ in range(n - 1):
        got.append(lax.ppermute(got[-1], axis, pairs))
    return got


def shards(wavefunction, start_block):
    sizes = rows_n, cols_n, layers = tuple(lax.axis_size(a) for a in ("row", "col", "layer"))
    row, col, layer = (lax.axis_index(a).astype(jnp.int32) for a in ("row", "col", "layer"))
    order_m = wavefunction.shape[0] * rows_n
    panel = start_block.shape[1]
    size = min(256, panel)
    per = panel // size
    place = jnp.stack([row, col, layer])

    width = wavefunction.shape[1] // layers
    own = lax.dynamic_slice_in_dim(wavefunction, layer * width, width, 1)
    chains = [(chain(cut, "row", 1), chain(cut, "row", -1)) for cut in jnp.split(own, 2)]
    blocks = [[c[0][0] for c in chains]]
    for s in range(1, rows_n):
        blocks += [[c[0][s] for c in chains], [c[1][s] for c in chains]]
    starts, s_places = [], []
    for s, part in enumerate(own_and_others(start_block, "col")):
        for t, piece in enumerate(own_and_others(part, "layer")):
            starts.append(piece)
            s_places.append((col ^ s) * layers + (layer ^ t))
    s_places = jnp.stack(s_places)
    inner = image_call(place, s_places, blocks[:-2], starts, sizes, per)
    images = image_call(place, s_places, blocks, starts, sizes, per, inner)
    panels = [[]]
    for h in range(per):
        image = exchange_sum([images[x * per + h] for x in range(layers)], "layer")
        panels[0].append(exchange_sum([image[s] for s in range(cols_n)], "col", 1 + h % 2))

    bundles = all_bundles(rows_n, per)
    up = [(a, a + 1) for a in range(rows_n - 1)]
    g_arrays = []
    for n, bundle in enumerate(bundles):
        s = bundle[-1][0]
        if s == len(panels):
            panels.append([])
            for h in range(per):
                panels[-1].append(lax.ppermute(panels[-2][h], "row", up))
        gram = gram_call(place, bundle, panels, (cols_n, layers))
        gram = exchange_sum(gram, "layer")
        gram = [gram[y] for y in range(cols_n)]
        gram = exchange_sum(gram, "col", 0 if n >= rows_n - 2 else 1)
        pieces = own_and_others(gram, "col", 0 if n > rows_n - 1 else 1 + n % 2)
        stack = jnp.stack(pieces)
        g_arrays.append(pieces + own_and_others(stack, "layer")[1:])
    places = jnp.stack([(layer ^ x) * cols_n + (col ^ s) for x in range(layers) for s in range(cols_n)])
    return factor_apply(place, places, bundles, g_arrays, cols_n, panels, size, math.sqrt(order_m))


def all_bundles(rows_n, per):
    whole = [[(s, h) for h in range(per)] for s in range(rows_n - 1)]
    return whole + [[(rows_n - 1, h)] for h in range(per)]


def solution(mesh):
    placed = (P("row", "col"), P(("col", "layer"), "row"))

    return jax.shard_map(shards, mesh=mesh, in_specs=placed, out_specs=P(("col", "layer"), "row"), check_vma=False)
```
